32 devices in a mesh: wave: 16 (over z, y, core), lev: 2 (over x).
Axes of the slice: x: 2, y: 2, z: 4, core: 2. Of those that a mesh axis runs over, the one named last changes fastest.
Arguments:
- control: bfloat16 [2, 256, 256, 2, 512], P(None, 'wave', 'lev'), may hold values from -6 to 6
- wave_of_slot: int32 [256], replicated, may hold values from 0 to 255, each once
- legendre: bfloat16 [256, 256, 256], P('wave', 'lev'), may hold values from -0.375 to 0.375
- vertical: bfloat16 [4, 4, 128, 128], replicated, may hold values from -0.5 to 0.5
- points: int32 [256], P('wave'), may hold values from 128 to 512
- lat_band: int32 [256], P('wave'), may hold values from 0 to 7, never falling along the last dimension, each value on 1 to 64 neighbouring positions
- grid_scale: float32 [8, 512], P(None, 'lev'), may hold values from 0.5 to 2
- obs_weight: bfloat16 [256, 512, 512], P('wave', 'lev'), may hold values from 0.19921875 to 1
Outputs:
- increment: bfloat16 [2, 256, 512, 512], P(None, 'wave', 'lev')
- gradient: bfloat16 [2, 256, 256, 2, 512], P(None, 'wave', 'lev')
The draws below stay inside these ranges and needn't reach their ends.
Inputs may be any that keep to these rules, and one draw needn't show every extreme that they name: `wave_of_slot`: each zonal wavenumber 0 to 255 stands in exactly one slot. `lat_band`: band numbers never fall from one latitude to the next, and each band covers 1 to 64 latitudes.
All inputs are finite; a program needn't handle non-finite values.
Results may differ from the reference program's by a relative error of at most 0.007.
Values may be sent and summed in bfloat16 or wider, within the bound.
A program may use at most 192 MiB of HBM per device.

```python
import math
import jax
import jax.numpy as jnp
import numpy as np

WAVES = 256
LATITUDES = 256
LONGITUDES = 512
LEVELS = 128
VARIABLES = 4
COV_BANDS = 4
LAT_BANDS = 8
MEMBERS = 2
COLUMNS = 512


def plant(drawn, own_key, least, top_value):
    index_at = [jax.random.randint(jax.random.fold_in(own_key, axis), (), 0, length) for axis, length in enumerate(drawn.shape)]
    widest = drawn.shape.index(max(drawn.shape))
    next_to = index_at[:widest] + [(index_at[widest] + 1) % drawn.shape[widest]] + index_at[widest + 1:]
    return drawn.at[tuple(index_at)].set(least).at[tuple(next_to)].set(top_value)


def level_of(stream_key, extent, shards, least, high):
    gain, own = 1.0, jax.random.fold_in(stream_key, 6)
    for position, blocks in shards:
        steps = jnp.exp(jax.random.uniform(jax.random.fold_in(own, position), (blocks,), jnp.float32, least / len(shards), high / len(shards)))
        gain = gain * jnp.repeat(steps, extent[position] // blocks).reshape([-1 if axis == position else 1 for axis in range(len(extent))])
    return gain


def length_profile(count, total, most, skew):
    portions = [(1 << 20) // math.isqrt(rank ** skew) + 1 for rank in range(2, count + 1)]
    rest, holding = total - most - (count - 1), [1] * (count - 1)
    while rest > 0:
        candidates = [i for i in range(count - 1) if holding[i] < most]
        whole, remaining = sum([portions[i] for i in candidates]), rest
        for i in candidates:
            more = min(most - holding[i], max(1, remaining * portions[i] // whole), rest)
            holding[i] = holding[i] + more
            rest = rest - more
    return np.array([most] + holding)


def ragged_sizes(rng, count, total, reach, slope):
    if count == 2:
        one = jax.random.randint(rng, (), max(1, total - reach), min(reach, total - 1) + 1)
        return jnp.stack([one, total - one])
    tallies = jnp.asarray(length_profile(count, total, reach, slope), jnp.int32)
    couples = (count - 1) // 2
    donor, receiver = tallies[1:1 + 2 * couples:2], tallies[2:2 + 2 * couples:2]
    slack = jnp.minimum(donor - 1, reach - receiver)
    passed = jax.random.randint(jax.random.fold_in(rng, 1), (couples,), 0, 1 << 20) % (slack + 1)
    tallies = tallies.at[1:1 + 2 * couples:2].set(donor - passed).at[2:2 + 2 * couples:2].set(receiver + passed)
    return tallies[jax.random.permutation(jax.random.fold_in(rng, 2), count)]


def scatter_about(key, dims, spread, most, pieces=(), held_as=jnp.bfloat16):
    drawn = jax.random.normal(key, dims, jnp.float32) * spread
    if len(pieces) > 0:
        drawn = level_of(key, dims, pieces, -0.22, 0.18) * drawn
    return jnp.clip(drawn, min=-most, max=most).astype(held_as)


def setup_inputs(seed: int = 0) -> dict:
    splits = jax.random.split(jax.random.key(seed), 9)
    return {
        "control": scatter_about(splits[0], (MEMBERS, WAVES, WAVES, 2, COLUMNS), 1.0, 6.0, ((1, 16), (2, 2))),
        "wave_of_slot": jax.random.permutation(splits[1], WAVES).astype(jnp.int32),
        "legendre": scatter_about(splits[2], (WAVES, WAVES, LATITUDES), WAVES ** -0.5, 0.375, ((0, 16), (1, 2))),
        "vertical": scatter_about(splits[3], (COV_BANDS, VARIABLES, LEVELS, LEVELS), LEVELS ** -0.5, 0.5),
        "points": plant(jax.random.randint(splits[4], (LATITUDES,), LONGITUDES // 4, LONGITUDES + 1), jax.random.fold_in(splits[4], 1), LONGITUDES // 4, LONGITUDES).astype(jnp.int32),
        "lat_band": jnp.searchsorted(jnp.cumsum(ragged_sizes(splits[5], LAT_BANDS, LATITUDES, 2 * LATITUDES // LAT_BANDS, 1)), jnp.arange(LATITUDES), side="right").astype(jnp.int32),
        "grid_scale": jnp.clip(jnp.exp(math.log(2.0) - 1.3862944 * jax.random.uniform(splits[6], (LAT_BANDS, COLUMNS), jnp.float32) ** level_of(splits[6], (LAT_BANDS, COLUMNS), ((1, 2),), -0.2, 0.2)), 0.5, 2.0),
        "obs_weight": jnp.clip(jnp.exp(math.log(1.0) - 1.6133518 * jax.random.uniform(splits[7], (LATITUDES, COLUMNS, LONGITUDES), jnp.float32) ** level_of(splits[7], (LATITUDES, COLUMNS, LONGITUDES), ((0, 16), (1, 2)), -0.2, 0.2)), 0.19921875, 1.0).astype(jnp.bfloat16),
    }


def fourier_table(wave_ids, lat_points):
    lon_index = jnp.arange(LONGITUDES, dtype=jnp.int32)
    remainder = wave_ids[None, :, None] * lon_index[None, None, :] % lat_points[:, None, None]
    angles = 2.0 * math.pi * remainder.astype(jnp.float32) / lat_points.astype(jnp.float32)[:, None, None]
    factor = jnp.where(wave_ids == 0, 1.0, 2.0).astype(jnp.float32) / math.sqrt(4.0 * WAVES)
    inside = lon_index[None, None, :] < lat_points[:, None, None]
    cosine = jnp.where(inside, factor[None, :, None] * jnp.cos(angles), 0.0)
    sine = jnp.where(inside, -factor[None, :, None] * jnp.sin(angles), 0.0)
    return jnp.stack([cosine, sine], axis=2).astype(jnp.bfloat16)

def vertical_apply(field, vertical, live_rows, band_of, forward):
    shaped = field.astype(jnp.float32).reshape(WAVES, WAVES, 2, VARIABLES, LEVELS)
    matrices = vertical.astype(jnp.float32)
    form = 'skpam,alm->skpal' if forward else 'skpal,alm->skpam'
    summed = jnp.zeros(shaped.shape, jnp.float32)
    for index_band in range(COV_BANDS):
        partial_value = jnp.einsum(form, shaped, matrices[index_band])
        chosen = live_rows & (band_of == index_band)
        summed = summed + jnp.where(chosen[:, :, None, None, None], partial_value, 0.0)
    return summed.reshape(WAVES, WAVES, 2, COLUMNS).astype(jnp.bfloat16)

def reference(control, wave_of_slot, legendre, vertical, points, lat_band, grid_scale, obs_weight):
    row_index = jnp.arange(WAVES, dtype=jnp.int32)
    totals_n = wave_of_slot[:, None] + row_index[None, :]
    live_rows = totals_n <= WAVES - 1
    band_of = jnp.minimum(totals_n * COV_BANDS // WAVES, COV_BANDS - 1)
    fourier = fourier_table(wave_of_slot, points).astype(jnp.float32)
    table32 = legendre.astype(jnp.float32)
    lat_scale = grid_scale[lat_band]
    weight32 = obs_weight.astype(jnp.float32)
    increments = []
    gradients = []
    for member in range(MEMBERS):
        spectral = vertical_apply(control[member], vertical, live_rows, band_of, True)
        flat = spectral.astype(jnp.float32).reshape(WAVES, WAVES, 2 * COLUMNS)
        coeffs = jnp.einsum('skt,skq->stq', table32, flat).astype(jnp.bfloat16)
        coeffs32 = coeffs.astype(jnp.float32).reshape(WAVES, LATITUDES, 2, COLUMNS)
        synthesis = jnp.einsum('tspj,stpc->tcj', fourier, coeffs32)
        increment = (synthesis * lat_scale[:, :, None]).astype(jnp.bfloat16)
        weighted = (increment.astype(jnp.float32) * weight32 * lat_scale[:, :, None]).astype(jnp.bfloat16)
        adjoint_fourier = jnp.einsum('tspj,tcj->tspc', fourier, weighted.astype(jnp.float32)).astype(jnp.bfloat16)
        adjoint_flat = adjoint_fourier.astype(jnp.float32).reshape(LATITUDES, WAVES, 2 * COLUMNS)
        adjoint_coeffs = jnp.einsum('skt,tsq->skq', table32, adjoint_flat).astype(jnp.bfloat16)
        adjoint_coeffs = adjoint_coeffs.reshape(WAVES, WAVES, 2, COLUMNS)
        gradient = vertical_apply(adjoint_coeffs, vertical, live_rows, band_of, False)
        increments.append(increment)
        gradients.append(gradient)
    return (jnp.stack(increments, axis=0), jnp.stack(gradients, axis=0))
```

```python
import functools
import math

import jax
import jax.numpy as jnp
from jax import lax
from jax.experimental import pallas as pl
from jax.experimental.pallas import tpu as pltpu
from jax.sharding import PartitionSpec as P

WAVES = 256
LONGITUDES = 512
LEVELS = 128
VARIABLES = 4
COV_BANDS = 4


def fourier_table(wave_ids, lat_points):
    lon_index = jnp.arange(LONGITUDES, dtype=jnp.int32)
    remainder = wave_ids[None, :, None] * lon_index[None, None, :] % lat_points[:, None, None]
    angles = (
        2.0
        * math.pi
        * remainder.astype(jnp.float32)
        / lat_points.astype(jnp.float32)[:, None, None]
    )
    factor = jnp.where(wave_ids == 0, 1.0, 2.0).astype(jnp.float32) / math.sqrt(4.0 * WAVES)
    inside = lon_index[None, None, :] < lat_points[:, None, None]
    cosine = jnp.where(inside, factor[None, :, None] * jnp.cos(angles), 0.0)
    sine = jnp.where(inside, -factor[None, :, None] * jnp.sin(angles), 0.0)
    return jnp.stack([cosine, sine], axis=2).astype(jnp.bfloat16)


def vertical_apply(field, vertical, live_rows, band_of, forward):
    members, slots, rows_dev = (field.shape[0], field.shape[1], field.shape[2])
    shaped = field.reshape(members, slots, rows_dev, 2, VARIABLES, LEVELS)
    form = "eskpam,alm->eskpal" if forward else "eskpal,alm->eskpam"
    summed = jnp.zeros(shaped.shape, jnp.float32)
    for index_band in range(COV_BANDS):
        partial_value = jnp.einsum(
            form, shaped, vertical[index_band], preferred_element_type=jnp.float32
        )
        chosen = live_rows & (band_of == index_band)
        summed = summed + jnp.where(chosen[None, :, :, None, None, None], partial_value, 0.0)
    return summed.reshape(field.shape).astype(jnp.bfloat16)


def to_bands(values):
    return lax.all_to_all(values, "wave", split_axis=2, concat_axis=1, tiled=True)


def shards_plain(control, wave_of_slot, legendre, vertical, points, lat_band, grid_scale, obs_weight):
    members, slots, rows_dev = (control.shape[0], control.shape[1], control.shape[2])
    slot_start = lax.axis_index("wave") * slots
    row_start = lax.axis_index("lev") * rows_dev
    own_waves = lax.dynamic_slice_in_dim(wave_of_slot, slot_start, slots)
    row_index = row_start + jnp.arange(rows_dev, dtype=jnp.int32)
    totals_n = own_waves[:, None] + row_index[None, :]
    live_rows = totals_n <= WAVES - 1
    band_of = jnp.minimum(totals_n * COV_BANDS // WAVES, COV_BANDS - 1)
    spectral = vertical_apply(control, vertical, live_rows, band_of, True)
    columns = lax.all_to_all(spectral, "lev", split_axis=4, concat_axis=2, tiled=True)
    col_dev = columns.shape[4]
    width = 2 * col_dev
    all_rows = columns.shape[2]
    columns = columns.reshape(members, slots, all_rows, width)
    coeffs = jnp.einsum(
        "skt,eskq->estq",
        lax.all_gather(legendre, "lev", axis=1, tiled=True),
        columns,
        preferred_element_type=jnp.float32,
    )
    coeffs = coeffs.astype(jnp.bfloat16)
    by_lat = to_bands(coeffs)
    wave_count = by_lat.shape[1]
    lat_dev = by_lat.shape[2]
    by_lat = by_lat.reshape(members, wave_count, lat_dev, 2, col_dev)
    fourier = fourier_table(wave_of_slot, points)
    synthesis = jnp.einsum("tspj,estpc->etcj", fourier, by_lat, preferred_element_type=jnp.float32)
    chooser = (
        lat_band[:, None] == jnp.arange(grid_scale.shape[0], dtype=jnp.int32)[None, :]
    ).astype(jnp.float32)
    lat_scale = jnp.dot(chooser, grid_scale, precision=lax.Precision.HIGHEST)
    increment = (synthesis * lat_scale[None, :, :, None]).astype(jnp.bfloat16)
    weighted = (
        increment.astype(jnp.float32) * obs_weight.astype(jnp.float32) * lat_scale[None, :, :, None]
    ).astype(jnp.bfloat16)
    adjoint_fourier = jnp.einsum(
        "tspj,etcj->etspc", fourier, weighted, preferred_element_type=jnp.float32
    )
    adjoint_fourier = adjoint_fourier.astype(jnp.bfloat16).reshape(
        members, lat_dev, wave_count, width
    )
    band_rows = to_bands(adjoint_fourier)
    adjoint_coeffs = jnp.einsum(
        "skt,etsq->eskq",
        lax.all_gather(legendre, "lev", axis=1, tiled=True),
        band_rows,
        preferred_element_type=jnp.float32,
    )
    adjoint_coeffs = adjoint_coeffs.astype(jnp.bfloat16).reshape(
        members, slots, all_rows, 2, col_dev
    )
    rows_back = lax.all_to_all(adjoint_coeffs, "lev", split_axis=2, concat_axis=4, tiled=True)
    gradient = vertical_apply(rows_back, vertical, live_rows, band_of, False)
    return (increment, gradient)


MESH = pl.DeviceIdType.MESH
VMEM_BYTES = 65000 * 1024
GROUPS = 2
RING = 4


def enter(n_wave, n_lev):
    me_w, me_l = lax.axis_index("wave"), lax.axis_index("lev")
    barrier = pltpu.get_barrier_semaphore()

    def greet(d, carry):
        peer = lax.rem(me_w + d, n_wave)
        pl.semaphore_signal(barrier, inc=1, device_id=(peer, me_l), device_id_type=MESH)
        return carry

    lax.fori_loop(1, n_wave, greet, 0)
    for d in range(1, n_lev):
        peer = lax.rem(me_l + d, n_lev)
        pl.semaphore_signal(barrier, inc=1, device_id=(me_w, peer), device_id_type=MESH)
    pl.semaphore_wait(barrier, n_wave + n_lev - 2)


def band_masks(total, waves):
    width = waves // COV_BANDS
    masks = []
    for b in range(COV_BANDS):
        hit = (total >= b * width) & (total < (b + 1) * width)
        masks.append(jnp.where(hit, 1.0, 0.0).astype(jnp.bfloat16))
    return masks


def banded_dot(x, masks, matrix):
    stacked = jnp.concatenate([x * mask for mask in masks], axis=1)
    return jnp.dot(stacked, matrix, preferred_element_type=jnp.float32)


SIN_TERMS = [(-1.0) ** i * (2.0 * math.pi) ** (2 * i + 1) / math.factorial(2 * i + 1) for i in range(10)]
COS_TERMS = [(-1.0) ** i * (2.0 * math.pi) ** (2 * i) / math.factorial(2 * i) for i in range(10)]


def horner(terms, square):
    value = jnp.full_like(square, terms[-1])
    for term in terms[-2::-1]:
        value = value * square + term
    return value


def loop(first, last, body):
    def step(i, carry):
        body(i)
        return carry

    lax.fori_loop(first, last, step, 0)


def transform_kernel(n_wave, n_lev, waves_ref, points_ref, order_ref, scale_ref, vf_ref, vg_ref, x_ref, l_ref, weight_ref,
                     inc_ref, grad_ref,
                     full, pieces, own, away, spec, back, flat, wsend, land, aland, table, wbuf, ibuf, stage,
                     full_sem, x_sem, weight_sem, inc_sem, grad_sem, l_send, l_recv, f_send, f_recv, b_send, b_recv,
                     w_send, w_recv, a_send, a_recv):
    members, slots, rows = x_ref.shape[:3]
    per = vf_ref.shape[0] // n_lev
    lats, cols, longs = weight_ref.shape
    waves = n_wave * slots
    lat_all = n_wave * lats
    chunks = members * per
    size = slots // GROUPS
    units = chunks * GROUPS
    me_w, me_l = lax.axis_index("wave"), lax.axis_index("lev")
    row0 = me_l * rows
    bf16, f32 = jnp.bfloat16, jnp.float32

    def where_is(u):
        q, g = lax.div(u, GROUPS), lax.rem(u, GROUPS)
        return q, g, lax.div(q, per), lax.rem(q, per)

    def level_block(d, i):
        a = lax.rem(me_l + d, n_lev) * per + i
        return a, pl.ds(pl.multiple_of(a * LEVELS, LEVELS), LEVELS)

    def group_slots(g):
        return pl.ds(pl.multiple_of(g * size, size), size)

    def x_copy(u, d):
        _, g, e, i = where_is(u)
        slot = lax.rem(u, 2)
        return pltpu.make_async_copy(
            x_ref.at[e, group_slots(g), :, :, level_block(d, i)[1]], pieces.at[slot, d], x_sem.at[slot, d])

    def grad_copy(u, d):
        _, g, e, i = where_is(u)
        slot = lax.rem(u, 2)
        return pltpu.make_async_copy(
            pieces.at[slot, d], grad_ref.at[e, group_slots(g), :, :, level_block(d, i)[1]], grad_sem.at[slot, d])

    def weight_copy(q):
        i = lax.rem(q, per)
        return pltpu.make_async_copy(
            weight_ref.at[:, pl.ds(pl.multiple_of(i * LEVELS, LEVELS), LEVELS), :], wbuf, weight_sem)

    def inc_copy(q):
        e, i = lax.div(q, per), lax.rem(q, per)
        return pltpu.make_async_copy(
            ibuf, inc_ref.at[e, :, pl.ds(pl.multiple_of(i * LEVELS, LEVELS), LEVELS), :], inc_sem)

    def full_copy():
        return pltpu.make_async_copy(l_ref, full.at[me_l], full_sem)

    def table_copy(g, d):
        peer = lax.rem(me_l + d, n_lev)
        return pltpu.make_async_remote_copy(
            src_ref=l_ref.at[group_slots(g)], dst_ref=full.at[me_l, group_slots(g)],
            send_sem=l_send.at[g, d - 1], recv_sem=l_recv.at[g, d - 1],
            device_id=(me_w, peer), device_id_type=MESH)

    def lev_copy(u, d, target, send_sem, recv_sem):
        peer = lax.rem(me_l + d, n_lev)
        return pltpu.make_async_remote_copy(
            src_ref=away.at[lax.rem(u, RING), d - 1], dst_ref=target.at[u, n_lev - d - 1],
            send_sem=send_sem.at[u, d - 1], recv_sem=recv_sem.at[u, d - 1],
            device_id=(me_w, peer), device_id_type=MESH)

    def out_copy(u, d):
        return lev_copy(u, d, spec, f_send, f_recv)

    def back_copy(u, d):
        return lev_copy(u, d, back, b_send, b_recv)

    def wave_copy(u, d, target, send_sem, recv_sem):
        peer = lax.rem(me_w + d, n_wave)
        return pltpu.make_async_remote_copy(
            src_ref=wsend.at[u, peer], dst_ref=target.at[u, me_w],
            send_sem=send_sem.at[u, d - 1], recv_sem=recv_sem.at[u, d - 1],
            device_id=(peer, me_l), device_id_type=MESH)

    def land_copy(u, d):
        return wave_copy(u, d, land, w_send, w_recv)

    def aland_copy(u, d):
        return wave_copy(u, d, aland, a_send, a_recv)

    lev_others = range(1, n_lev)
    lev_order = list(lev_others) + [0]

    def vertical(u):
        _, g, e, i = where_is(u)
        slot, keep = lax.rem(u, 2), lax.rem(u, RING)
        for d in range(n_lev):
            x_copy(u, d).wait()

        @pl.when(u >= RING)
        def _():
            for d in lev_others:
                out_copy(u - RING, d).wait_send()

        def one(s):
            wave = waves_ref[g * size + s]
            total = wave + row0 + lax.div(lax.broadcasted_iota(jnp.int32, (2 * rows, LEVELS), 0), 2)
            masks = band_masks(total, waves)
            for d in lev_order:
                a, _ = level_block(d, i)
                x = pieces.at[slot, d].reshape(size, 2 * rows, LEVELS)[s]
                stage[d] = banded_dot(x, masks, vf_ref[a])
                for p in range(2):
                    y = stage[d, pl.ds(p, rows, stride=2), :].astype(bf16)
                    if d == 0:
                        own[keep, s, :, p * LEVELS:(p + 1) * LEVELS] = y
                    else:
                        away[keep, d - 1, s, :, p * LEVELS:(p + 1) * LEVELS] = y

        loop(0, size, one)
        for d in lev_others:
            out_copy(u, d).start()

        @pl.when(u + 2 < units)
        def _():
            for d in range(n_lev):
                x_copy(u + 2, d).start()

        @pl.when(u + 1 < GROUPS)
        def _():
            for d in lev_others:
                table_copy(u + 1, d).start()

    def legendre(u):
        _, g, e, i = where_is(u)
        keep = lax.rem(u, RING)
        coef = flat.reshape(size, lat_all, 2 * LEVELS)

        @pl.when(u == 0)
        def _():
            full_copy().wait()

        @pl.when(u < GROUPS)
        def _():
            for d in lev_others:
                table_copy(u, d).wait()

        for d in lev_others:
            out_copy(u, d).wait_recv()

        def one(s):
            fields, tables = [], []
            for d in range(n_lev):
                fields.append(own[keep, s] if d == 0 else spec[u, d - 1, s])
                tables.append(full[lax.rem(me_l + d, n_lev), g * size + s])
            coef[s] = lax.dot_general(
                jnp.concatenate(tables, axis=0), jnp.concatenate(fields, axis=0),
                (((0,), (0,)), ((), ())), preferred_element_type=f32)

        loop(0, size, one)

        def turn(w):
            for t in range(lats):
                wsend[u, w, t] = coef[:, w * lats + t, :].astype(bf16)

        loop(0, n_wave, turn)
        loop(1, n_wave, lambda d: land_copy(u, d).start())
        land[u, me_w] = wsend[u, me_w]

    def build(t):
        points = points_ref[t]
        n = points.astype(f32)
        piece = 32
        inverse = 1.0 / jnp.full((1, longs), n, f32)
        lane = lax.broadcasted_iota(jnp.int32, (1, longs), 1)
        inside = jnp.where(lane < points, 1.0, 0.0) / math.sqrt(4.0 * waves)

        def some(k):
            base = pl.multiple_of(k * piece, piece)
            wave = order_ref[pl.ds(base, piece), :]
            product = wave * lane.astype(f32)
            turns = jnp.floor(product * inverse + 0.5)
            x = (product - turns * n) * inverse
            square = x * x
            gain = jnp.where(wave == 0.0, 1.0, 2.0) * inside
            table[t, pl.ds(base, piece), :] = (gain * horner(COS_TERMS, square)).astype(bf16)
            sine = (-gain) * (x * horner(SIN_TERMS, square))
            table[t, pl.ds(pl.multiple_of(waves + base, piece), piece), :] = sine.astype(bf16)

        loop(0, waves // piece, some)

    def grid(q):
        i = lax.rem(q, per)
        weight_copy(q).wait()

        @pl.when(q > 0)
        def _():
            inc_copy(q - 1).wait()

        for g in range(GROUPS):
            loop(1, n_wave, lambda d: land_copy(q * GROUPS + g, d).wait())
        here = pl.ds(q * GROUPS, GROUPS)
        scales = scale_ref[pl.ds(pl.multiple_of(i * LEVELS, LEVELS), LEVELS), :]
        column = lax.broadcasted_iota(jnp.int32, scales.shape, 1)

        def one(t):
            scale = jnp.sum(jnp.where(column == t, scales, 0.0), axis=1, keepdims=True)
            parts = [land[here, :, t, :, p * LEVELS:(p + 1) * LEVELS].reshape(waves, LEVELS) for p in range(2)]
            synthesis = lax.dot_general(jnp.concatenate(parts, axis=0), table[t], (((0,), (0,)), ((), ())),
                                        preferred_element_type=f32)
            increment = (synthesis * scale).astype(bf16)
            ibuf[t] = increment
            weighted = increment.astype(f32) * wbuf[t].astype(f32) * scale
            adjoint = lax.dot_general(table[t], weighted.astype(bf16), (((1,), (1,)), ((), ())),
                                      preferred_element_type=f32).astype(bf16)
            for p in range(2):
                part = adjoint[p * waves:(p + 1) * waves].reshape(GROUPS, n_wave, size, LEVELS)
                wsend[here, :, t, :, p * LEVELS:(p + 1) * LEVELS] = part

        loop(0, lats, one)
        for g in range(GROUPS):
            u = q * GROUPS + g
            loop(1, n_wave, lambda d: aland_copy(u, d).start())
            aland[u, me_w] = wsend[u, me_w]
        inc_copy(q).start()

        @pl.when(q + 1 < chunks)
        def _():
            weight_copy(q + 1).start()

    def adjoint_legendre(u):
        _, g, e, i = where_is(u)
        keep = lax.rem(u, RING)
        fine = flat.reshape(lat_all, size, 2 * LEVELS)
        loop(1, n_wave, lambda d: aland_copy(u, d).wait())

        @pl.when(u < RING)
        def _():
            for d in lev_others:
                out_copy(u + units - RING, d).wait_send()

        @pl.when(u >= RING)
        def _():
            for d in lev_others:
                back_copy(u - RING, d).wait_send()

        def widen(w):
            fine[pl.ds(pl.multiple_of(w * lats, lats), lats)] = aland[u, w].astype(f32)

        loop(0, n_wave, widen)

        def one(s):
            field = fine[:, s, :].astype(bf16)
            for d in lev_order:
                y = jnp.dot(full[lax.rem(me_l + d, n_lev), g * size + s], field, preferred_element_type=f32).astype(bf16)
                if d == 0:
                    own[keep, s] = y
                else:
                    away[keep, d - 1, s] = y

        loop(0, size, one)
        for d in lev_others:
            back_copy(u, d).start()

    def adjoint_vertical(u):
        _, g, e, i = where_is(u)
        slot, keep = lax.rem(u, 2), lax.rem(u, RING)
        for d in lev_others:
            back_copy(u, d).wait_recv()

        @pl.when(u >= 2)
        def _():
            for d in range(n_lev):
                grad_copy(u - 2, d).wait()

        def one(s):
            wave = waves_ref[g * size + s]
            masks = band_masks(wave + row0 + lax.broadcasted_iota(jnp.int32, (rows, LEVELS), 0), waves)
            for d in range(n_lev):
                a, _ = level_block(d, i)
                for p in range(2):
                    at = slice(p * LEVELS, (p + 1) * LEVELS)
                    x = own[keep, s, :, at] if d == 0 else back[u, d - 1, s, :, at]
                    stage[d, pl.ds(p, rows, stride=2), :] = banded_dot(x, masks, vg_ref[a])
                pieces.at[slot, d].reshape(size, 2 * rows, LEVELS)[s] = stage[d].astype(bf16)

        loop(0, size, one)
        for d in range(n_lev):
            grad_copy(u, d).start()

    ahead = RING - 1
    full_copy().start()
    for u in range(2):
        for d in range(n_lev):
            x_copy(u, d).start()
    weight_copy(0).start()
    enter(n_wave, n_lev)
    for d in lev_others:
        table_copy(0, d).start()
    loop(0, ahead, vertical)
    loop(0, lats // 2, build)

    def front(u):
        legendre(u)
        vertical(u + ahead)

        @pl.when(u == 0)
        def _():
            loop(lats // 2, lats, build)

    loop(0, units - ahead, front)
    loop(units - ahead, units, legendre)
    loop(0, chunks, grid)
    adjoint_legendre(0)

    def tail(u):
        adjoint_legendre(u + 1)
        adjoint_vertical(u)

    loop(0, units - 1, tail)
    adjoint_vertical(units - 1)
    inc_copy(chunks - 1).wait()
    for u in range(units - 2, units):
        for d in range(n_lev):
            grad_copy(u, d).wait()
    for u in range(units - RING, units):
        for d in lev_others:
            back_copy(u, d).wait_send()


def shards_kernel(n_wave, n_lev, control, wave_of_slot, legendre, vertical, points, lat_band, grid_scale, obs_weight):
    members, slots, rows = control.shape[:3]
    waves = wave_of_slot.shape[0]
    variables = vertical.shape[1]
    columns = control.shape[4]
    cols = columns // n_lev
    lats, _, longs = obs_weight.shape
    per = variables // n_lev
    chunks = members * per
    size = slots // GROUPS
    units = chunks * GROUPS
    bf16, f32 = jnp.bfloat16, jnp.float32
    own_waves = lax.dynamic_slice_in_dim(wave_of_slot, lax.axis_index("wave") * slots, slots)
    order = wave_of_slot.reshape(n_wave, GROUPS, size).transpose(1, 0, 2).reshape(waves, 1).astype(f32)
    stack_f = vertical.transpose(1, 0, 3, 2).reshape(variables, COV_BANDS * LEVELS, LEVELS)
    stack_g = vertical.transpose(1, 0, 2, 3).reshape(variables, COV_BANDS * LEVELS, LEVELS)
    chooser = (
        lat_band[:, None] == jnp.arange(grid_scale.shape[0], dtype=jnp.int32)[None, :]
    ).astype(f32)
    lat_scale = jnp.dot(chooser, grid_scale, precision=lax.Precision.HIGHEST).T
    vmem = pl.BlockSpec(memory_space=pltpu.VMEM)
    smem = pl.BlockSpec(memory_space=pltpu.SMEM)
    hbm = pl.BlockSpec(memory_space=pl.ANY)
    dma = pltpu.SemaphoreType.DMA
    others = n_lev - 1
    half = (size, rows, 2 * LEVELS)
    packet = (units, n_wave, lats, size, 2 * LEVELS)
    return pl.pallas_call(
        functools.partial(transform_kernel, n_wave, n_lev),
        out_shape=[
            jax.ShapeDtypeStruct((members, lats, cols, longs), bf16),
            jax.ShapeDtypeStruct(control.shape, bf16),
        ],
        in_specs=[smem, smem, vmem, vmem, vmem, vmem, hbm, hbm, hbm],
        out_specs=[hbm, hbm],
        scratch_shapes=[
            pltpu.VMEM((n_lev, *legendre.shape), bf16),
            pltpu.VMEM((2, n_lev, size, rows, 2, LEVELS), bf16),
            pltpu.VMEM((RING, *half), bf16),
            pltpu.VMEM((RING, others, *half), bf16),
            pltpu.VMEM((units, others, *half), bf16),
            pltpu.VMEM((units, others, *half), bf16),
            pltpu.VMEM((size * n_wave * lats, 2 * LEVELS), f32),
            pltpu.VMEM(packet, bf16),
            pltpu.VMEM(packet, bf16),
            pltpu.VMEM(packet, bf16),
            pltpu.VMEM((lats, 2 * waves, longs), bf16),
            pltpu.VMEM((lats, LEVELS, longs), bf16),
            pltpu.VMEM((lats, LEVELS, longs), bf16),
            pltpu.VMEM((n_lev, 2 * rows, LEVELS), f32),
            dma, dma((2, n_lev)), dma, dma, dma((2, n_lev)),
            dma((GROUPS, others)), dma((GROUPS, others)),
            dma((units, others)), dma((units, others)), dma((units, others)), dma((units, others)),
            dma((units, n_wave - 1)), dma((units, n_wave - 1)), dma((units, n_wave - 1)), dma((units, n_wave - 1)),
        ],
        compiler_params=pltpu.CompilerParams(collective_id=0, has_side_effects=True, vmem_limit_bytes=VMEM_BYTES),
        name="transform",
    )(own_waves, points, order, lat_scale, stack_f, stack_g, control, legendre, obs_weight)


def shards(n_wave, n_lev, *arrays):
    slots, rows, columns = arrays[0].shape[1], arrays[0].shape[2], arrays[0].shape[4]
    whole_tiles = slots % 16 == 0 and rows % 128 == 0 and columns % (n_lev * LEVELS) == 0
    if whole_tiles and n_lev > 1:
        return shards_kernel(n_wave, n_lev, *arrays)
    return shards_plain(*arrays)


def solution(mesh):
    in_specs = (
        P(None, "wave", "lev", None, None),
        P(),
        P("wave", "lev", None),
        P(),
        P("wave"),
        P("wave"),
        P(None, "lev"),
        P("wave", "lev", None),
    )
    out_specs = (P(None, "wave", "lev", None), P(None, "wave", "lev", None, None))
    body = functools.partial(shards, mesh.shape["wave"], mesh.shape["lev"])
    return jax.shard_map(body, mesh=mesh, in_specs=in_specs, out_specs=out_specs, check_vma=False)
```

```python
import functools
import math

import jax
import jax.numpy as jnp
from jax import lax
from jax.experimental import pallas as pl
from jax.experimental.pallas import tpu as pltpu
from jax.sharding import PartitionSpec as P

WAVES = 256
LONGITUDES = 512
LEVELS = 128
VARIABLES = 4
COV_BANDS = 4


def fourier_table(wave_ids, lat_points):
    lon_index = jnp.arange(LONGITUDES, dtype=jnp.int32)
    remainder = wave_ids[None, :, None] * lon_index[None, None, :] % lat_points[:, None, None]
    angles = (
        2.0
        * math.pi
        * remainder.astype(jnp.float32)
        / lat_points.astype(jnp.float32)[:, None, None]
    )
    factor = jnp.where(wave_ids == 0, 1.0, 2.0).astype(jnp.float32) / math.sqrt(4.0 * WAVES)
    inside = lon_index[None, None, :] < lat_points[:, None, None]
    cosine = jnp.where(inside, factor[None, :, None] * jnp.cos(angles), 0.0)
    sine = jnp.where(inside, -factor[None, :, None] * jnp.sin(angles), 0.0)
    return jnp.stack([cosine, sine], axis=2).astype(jnp.bfloat16)


def vertical_apply(field, vertical, live_rows, band_of, forward):
    members, slots, rows_dev = (field.shape[0], field.shape[1], field.shape[2])
    shaped = field.reshape(members, slots, rows_dev, 2, VARIABLES, LEVELS)
    form = "eskpam,alm->eskpal" if forward else "eskpal,alm->eskpam"
    summed = jnp.zeros(shaped.shape, jnp.float32)
    for index_band in range(COV_BANDS):
        partial_value = jnp.einsum(
            form, shaped, vertical[index_band], preferred_element_type=jnp.float32
        )
        chosen = live_rows & (band_of == index_band)
        summed = summed + jnp.where(chosen[None, :, :, None, None, None], partial_value, 0.0)
    return summed.reshape(field.shape).astype(jnp.bfloat16)


def to_bands(values):
    return lax.all_to_all(values, "wave", split_axis=2, concat_axis=1, tiled=True)


def shards_plain(control, wave_of_slot, legendre, vertical, points, lat_band, grid_scale, obs_weight):
    members, slots, rows_dev = (control.shape[0], control.shape[1], control.shape[2])
    slot_start = lax.axis_index("wave") * slots
    row_start = lax.axis_index("lev") * rows_dev
    own_waves = lax.dynamic_slice_in_dim(wave_of_slot, slot_start, slots)
    row_index = row_start + jnp.arange(rows_dev, dtype=jnp.int32)
    totals_n = own_waves[:, None] + row_index[None, :]
    live_rows = totals_n <= WAVES - 1
    band_of = jnp.minimum(totals_n * COV_BANDS // WAVES, COV_BANDS - 1)
    spectral = vertical_apply(control, vertical, live_rows, band_of, True)
    columns = lax.all_to_all(spectral, "lev", split_axis=4, concat_axis=2, tiled=True)
    col_dev = columns.shape[4]
    width = 2 * col_dev
    all_rows = columns.shape[2]
    columns = columns.reshape(members, slots, all_rows, width)
    coeffs = jnp.einsum(
        "skt,eskq->estq",
        lax.all_gather(legendre, "lev", axis=1, tiled=True),
        columns,
        preferred_element_type=jnp.float32,
    )
    coeffs = coeffs.astype(jnp.bfloat16)
    by_lat = to_bands(coeffs)
    wave_count = by_lat.shape[1]
    lat_dev = by_lat.shape[2]
    by_lat = by_lat.reshape(members, wave_count, lat_dev, 2, col_dev)
    fourier = fourier_table(wave_of_slot, points)
    synthesis = jnp.einsum("tspj,estpc->etcj", fourier, by_lat, preferred_element_type=jnp.float32)
    chooser = (
        lat_band[:, None] == jnp.arange(grid_scale.shape[0], dtype=jnp.int32)[None, :]
    ).astype(jnp.float32)
    lat_scale = jnp.dot(chooser, grid_scale, precision=lax.Precision.HIGHEST)
    increment = (synthesis * lat_scale[None, :, :, None]).astype(jnp.bfloat16)
    weighted = (
        increment.astype(jnp.float32) * obs_weight.astype(jnp.float32) * lat_scale[None, :, :, None]
    ).astype(jnp.bfloat16)
    adjoint_fourier = jnp.einsum(
        "tspj,etcj->etspc", fourier, weighted, preferred_element_type=jnp.float32
    )
    adjoint_fourier = adjoint_fourier.astype(jnp.bfloat16).reshape(
        members, lat_dev, wave_count, width
    )
    band_rows = to_bands(adjoint_fourier)
    adjoint_coeffs = jnp.einsum(
        "skt,etsq->eskq",
        lax.all_gather(legendre, "lev", axis=1, tiled=True),
        band_rows,
        preferred_element_type=jnp.float32,
    )
    adjoint_coeffs = adjoint_coeffs.astype(jnp.bfloat16).reshape(
        members, slots, all_rows, 2, col_dev
    )
    rows_back = lax.all_to_all(adjoint_coeffs, "lev", split_axis=2, concat_axis=4, tiled=True)
    gradient = vertical_apply(rows_back, vertical, live_rows, band_of, False)
    return (increment, gradient)


MESH = pl.DeviceIdType.MESH
VMEM_BYTES = 65000 * 1024
PAIR = 2
RING = 8
AHEAD = 4
PIECES = 4


def greet(n_wave, n_lev):
    me_w, me_l = lax.axis_index("wave"), lax.axis_index("lev")
    barrier = pltpu.get_barrier_semaphore()

    def one(d, carry):
        peer = lax.rem(me_w + d, n_wave)
        pl.semaphore_signal(barrier, inc=1, device_id=(peer, me_l), device_id_type=MESH)
        return carry

    lax.fori_loop(1, n_wave, one, 0)
    for d in range(1, n_lev):
        peer = lax.rem(me_l + d, n_lev)
        pl.semaphore_signal(barrier, inc=1, device_id=(me_w, peer), device_id_type=MESH)
    return barrier


def band_masks(total, waves):
    width = waves // COV_BANDS
    masks = []
    for b in range(COV_BANDS):
        hit = (total >= b * width) & (total < (b + 1) * width)
        masks.append(jnp.where(hit, 1.0, 0.0).astype(jnp.bfloat16))
    return masks


def banded_dot(x, masks, matrix):
    stacked = jnp.concatenate([x * mask for mask in masks], axis=1)
    return jnp.dot(stacked, matrix, preferred_element_type=jnp.float32)


SIN_TERMS = [(-1.0) ** i * (2.0 * math.pi) ** (2 * i + 1) / math.factorial(2 * i + 1) for i in range(10)]
COS_TERMS = [(-1.0) ** i * (2.0 * math.pi) ** (2 * i) / math.factorial(2 * i) for i in range(10)]


def horner(terms, square):
    value = jnp.full_like(square, terms[-1])
    for term in terms[-2::-1]:
        value = value * square + term
    return value


def loop(first, last, body):
    def step(i, carry):
        body(i)
        return carry

    lax.fori_loop(first, last, step, 0)


def transform_kernel(n_wave, n_lev, waves_ref, points_ref, band_ref, grid_scale_ref, v_ref, x_ref, l_ref, weight_ref,
                     inc_ref, grad_ref,
                     full, mats, mats_t, order, pieces, own, away, spec, back, coef, wsend, asend, land, aland, table, wbuf, ibuf, stage,
                     full_sem, mats_sem, x_sem, weight_sem, inc_sem, grad_sem, l_send, l_recv, f_send, f_recv, b_send, b_recv,
                     w_send, w_recv, a_send, a_recv):
    members, slots, rows = x_ref.shape[:3]
    variables = v_ref.shape[1]
    per = variables // n_lev
    lats, cols, longs = weight_ref.shape
    waves = n_wave * slots
    lat_all = n_wave * lats
    chunks = members * per
    subs = slots // PAIR
    units = chunks * subs
    me_w, me_l = lax.axis_index("wave"), lax.axis_index("lev")
    row0 = me_l * rows
    bf16, f32 = jnp.bfloat16, jnp.float32

    def where_is(u):
        q, g = lax.div(u, subs), lax.rem(u, subs)
        return q, g, lax.div(q, per), lax.rem(q, per)

    def level_block(d, i):
        a = lax.rem(me_l + d, n_lev) * per + i
        return a, pl.ds(pl.multiple_of(a * LEVELS, LEVELS), LEVELS)

    def pair_slots(g):
        return pl.ds(g * PAIR, PAIR)

    def x_copy(u, d):
        _, g, e, i = where_is(u)
        slot = lax.rem(u, PIECES)
        return pltpu.make_async_copy(
            x_ref.at[e, pair_slots(g), :, :, level_block(d, i)[1]], pieces.at[slot, d], x_sem.at[slot, d])

    def grad_copy(u, d):
        _, g, e, i = where_is(u)
        slot = lax.rem(u, PIECES)
        return pltpu.make_async_copy(
            pieces.at[slot, d], grad_ref.at[e, pair_slots(g), :, :, level_block(d, i)[1]], grad_sem.at[slot, d])

    def weight_copy(q):
        i = lax.rem(q, per)
        return pltpu.make_async_copy(
            weight_ref.at[:, pl.ds(pl.multiple_of(i * LEVELS, LEVELS), LEVELS), :], wbuf, weight_sem)

    def inc_copy(q):
        e, i = lax.div(q, per), lax.rem(q, per)
        return pltpu.make_async_copy(
            ibuf, inc_ref.at[e, :, pl.ds(pl.multiple_of(i * LEVELS, LEVELS), LEVELS), :], inc_sem)

    def full_copy():
        return pltpu.make_async_copy(l_ref, full.at[me_l], full_sem)

    def mats_copy():
        return pltpu.make_async_copy(v_ref, mats, mats_sem)

    def table_copy(g, d):
        peer = lax.rem(me_l + d, n_lev)
        return pltpu.make_async_remote_copy(
            src_ref=l_ref.at[pair_slots(g)], dst_ref=full.at[me_l, pair_slots(g)],
            send_sem=l_send.at[g, d - 1], recv_sem=l_recv.at[g, d - 1],
            device_id=(me_w, peer), device_id_type=MESH)

    def lev_copy(u, d, target, send_sem, recv_sem):
        peer = lax.rem(me_l + d, n_lev)
        return pltpu.make_async_remote_copy(
            src_ref=away.at[lax.rem(u, RING), d - 1], dst_ref=target.at[u, n_lev - d - 1],
            send_sem=send_sem.at[u, d - 1], recv_sem=recv_sem.at[u, d - 1],
            device_id=(me_w, peer), device_id_type=MESH)

    def out_copy(u, d):
        return lev_copy(u, d, spec, f_send, f_recv)

    def back_copy(u, d):
        return lev_copy(u, d, back, b_send, b_recv)

    def remote(src, dst, send_sem, recv_sem, d):
        return pltpu.make_async_remote_copy(
            src_ref=src, dst_ref=dst, send_sem=send_sem, recv_sem=recv_sem,
            device_id=(lax.rem(me_w + d, n_wave), me_l), device_id_type=MESH)

    def land_copy(u, d):
        q, g, _, _ = where_is(u)
        peer = lax.rem(me_w + d, n_wave)
        return remote(wsend.at[q, g, :, peer], land.at[q, :, :, g, me_w], w_send.at[u], w_recv.at[u], d)

    def land_all(u):
        q, g, _, _ = where_is(u)
        most = pl.ds(0, n_wave - 1)
        return remote(wsend.at[q, g, :, most], land.at[q, :, :, g, most], w_send.at[u], w_recv.at[u], 1)

    def aland_copy(u, d):
        q, g, _, _ = where_is(u)
        peer = lax.rem(me_w + d, n_wave)
        return remote(asend.at[q, :, :, g, peer], aland.at[u, :, me_w], a_send.at[u], a_recv.at[u], d)

    def aland_all(u):
        q, g, _, _ = where_is(u)
        most = pl.ds(0, n_wave - 1)
        return remote(asend.at[q, :, :, g, most], aland.at[u, :, most], a_send.at[u], a_recv.at[u], 1)

    lev_others = range(1, n_lev)
    lev_order = list(lev_others) + [0]

    def own_wave(g, s):
        return waves_ref[me_w * slots + g * PAIR + s]

    def vertical(u):
        _, g, e, i = where_is(u)
        slot, keep = lax.rem(u, PIECES), lax.rem(u, RING)
        for d in range(n_lev):
            x_copy(u, d).wait()

        @pl.when(u >= RING)
        def _():
            for d in lev_others:
                out_copy(u - RING, d).wait_send()

        for s in range(PAIR):
            total = own_wave(g, s) + row0 + lax.div(lax.broadcasted_iota(jnp.int32, (2 * rows, LEVELS), 0), 2)
            masks = band_masks(total, waves)
            for d in lev_order:
                a, _ = level_block(d, i)
                x = pieces.at[slot, d].reshape(PAIR, 2 * rows, LEVELS)[s]
                stage[s, d] = banded_dot(x, masks, mats_t[a])
                for p in range(2):
                    y = stage[s, d, pl.ds(p, rows, stride=2), :].astype(bf16)
                    if d == 0:
                        own[keep, s, :, p * LEVELS:(p + 1) * LEVELS] = y
                    else:
                        away[keep, d - 1, s, :, p * LEVELS:(p + 1) * LEVELS] = y

        @pl.when(u + PIECES < units)
        def _():
            for d in range(n_lev):
                x_copy(u + PIECES, d).start()

    def send_levels(u):
        for d in lev_others:
            out_copy(u, d).start()

        @pl.when(u + 1 < subs)
        def _():
            for d in lev_others:
                table_copy(u + 1, d).start()

    def legendre(u):
        q, g, e, i = where_is(u)
        keep = lax.rem(u, RING)

        @pl.when(u == 0)
        def _():
            full_copy().wait()

        @pl.when(u < subs)
        def _():
            for d in lev_others:
                table_copy(u, d).wait()

        for d in lev_others:
            out_copy(u, d).wait_recv()

        for s in range(PAIR):
            fields, tables = [], []
            for d in range(n_lev):
                fields.append(own[keep, s] if d == 0 else spec[u, d - 1, s])
                tables.append(full[lax.rem(me_l + d, n_lev), g * PAIR + s])
            value = lax.dot_general(
                jnp.concatenate(tables, axis=0), jnp.concatenate(fields, axis=0),
                (((0,), (0,)), ((), ())), preferred_element_type=f32)
            for p in range(2):
                coef[p, pl.ds(s, lat_all, stride=PAIR), :] = value[:, p * LEVELS:(p + 1) * LEVELS]
        for p in range(2):
            wsend.at[q, g, p].reshape(lat_all * PAIR, LEVELS)[...] = coef[p].astype(bf16)
        loop(1, n_wave, lambda d: land_copy(u, d).start())
        land[q, :, :, g, me_w] = wsend[q, g, :, me_w]

    def make_order():
        def some(k):
            row = lax.broadcasted_iota(jnp.int32, (8, LEVELS), 0)
            values = jnp.zeros((8, LEVELS), jnp.int32)
            for j in range(8):
                r = k * 8 + j
                g, w, s = lax.div(r, n_wave * PAIR), lax.rem(lax.div(r, PAIR), n_wave), lax.rem(r, PAIR)
                values = jnp.where(row == j, waves_ref[w * slots + g * PAIR + s], values)
            order[pl.ds(pl.multiple_of(k * 8, 8), 8), :] = values.astype(f32)

        loop(0, waves // 8, some)

    def build(t):
        points = points_ref[t]
        n = points.astype(f32)
        piece = 32
        inverse = 1.0 / jnp.full((1, longs), n, f32)
        lane = lax.broadcasted_iota(jnp.int32, (1, longs), 1)
        inside = jnp.where(lane < points, 1.0, 0.0) / math.sqrt(4.0 * waves)

        def some(k):
            base = pl.multiple_of(k * piece, piece)
            wave = order[pl.ds(base, piece), 0:1]
            product = wave * lane.astype(f32)
            turns = jnp.floor(product * inverse + 0.5)
            x = (product - turns * n) * inverse
            square = x * x
            gain = jnp.where(wave == 0.0, 1.0, 2.0) * inside
            table[t, pl.ds(base, piece), :] = (gain * horner(COS_TERMS, square)).astype(bf16)
            sine = (-gain) * (x * horner(SIN_TERMS, square))
            table[t, pl.ds(pl.multiple_of(waves + base, piece), piece), :] = sine.astype(bf16)

        loop(0, waves // piece, some)

    def scale_column(t, i):
        block = grid_scale_ref[:, pl.ds(pl.multiple_of(i * LEVELS, LEVELS), LEVELS)]
        band = lax.broadcasted_iota(jnp.int32, block.shape, 0)
        line = jnp.sum(jnp.where(band == band_ref[t], block, 0.0), axis=0, keepdims=True)
        square = (LEVELS, LEVELS)
        diagonal = lax.broadcasted_iota(jnp.int32, square, 0) == lax.broadcasted_iota(jnp.int32, square, 1)
        return jnp.sum(jnp.where(diagonal, line, 0.0), axis=1, keepdims=True)

    def grid(q):
        i = lax.rem(q, per)
        weight_copy(q).wait()

        @pl.when(q > 0)
        def _():
            inc_copy(q - 1).wait()

        loop(0, subs, lambda g: land_all(q * subs + g).wait())

        def one(t):
            scale = scale_column(t, i)
            parts = [land.at[q, p, t].reshape(waves, LEVELS)[...] for p in range(2)]
            synthesis = lax.dot_general(jnp.concatenate(parts, axis=0), table[t], (((0,), (0,)), ((), ())),
                                        preferred_element_type=f32)
            increment = (synthesis * scale).astype(bf16)
            ibuf[t] = increment
            weighted = increment.astype(f32) * wbuf[t].astype(f32) * scale
            adjoint = lax.dot_general(table[t], weighted.astype(bf16), (((1,), (1,)), ((), ())),
                                      preferred_element_type=f32).astype(bf16)
            for p in range(2):
                asend.at[q, p, t].reshape(waves, LEVELS)[...] = adjoint[p * waves:(p + 1) * waves]

        loop(0, lats, one)

        def send(g):
            u = q * subs + g
            loop(1, n_wave, lambda d: aland_copy(u, d).start())
            aland[u, :, me_w] = asend[q, :, :, g, me_w]

        loop(0, subs, send)
        inc_copy(q).start()

        @pl.when(q + 1 < chunks)
        def _():
            weight_copy(q + 1).start()

    def adjoint_legendre(u):
        _, g, e, i = where_is(u)
        keep = lax.rem(u, RING)
        aland_all(u).wait()

        @pl.when(u < RING)
        def _():
            for d in lev_others:
                out_copy(u + units - RING, d).wait_send()

        @pl.when(u >= RING)
        def _():
            for d in lev_others:
                back_copy(u - RING, d).wait_send()

        for p in range(2):
            coef[p] = aland.at[u, p].reshape(lat_all * PAIR, LEVELS)[...].astype(f32)
        for s in range(PAIR):
            field = jnp.concatenate(
                [coef[p, pl.ds(s, lat_all, stride=PAIR), :].astype(bf16) for p in range(2)], axis=1)
            for d in lev_order:
                y = jnp.dot(full[lax.rem(me_l + d, n_lev), g * PAIR + s], field, preferred_element_type=f32).astype(bf16)
                if d == 0:
                    own[keep, s] = y
                else:
                    away[keep, d - 1, s] = y
        for d in lev_others:
            back_copy(u, d).start()

    def adjoint_vertical(u):
        _, g, e, i = where_is(u)
        slot, keep = lax.rem(u, PIECES), lax.rem(u, RING)
        for d in lev_others:
            back_copy(u, d).wait_recv()

        @pl.when(u >= PIECES)
        def _():
            for d in range(n_lev):
                grad_copy(u - PIECES, d).wait()

        for s in range(PAIR):
            masks = band_masks(own_wave(g, s) + row0 + lax.broadcasted_iota(jnp.int32, (rows, LEVELS), 0), waves)
            for d in range(n_lev):
                a, _ = level_block(d, i)
                matrix = mats[:, a].reshape(COV_BANDS * LEVELS, LEVELS)
                for p in range(2):
                    at = slice(p * LEVELS, (p + 1) * LEVELS)
                    x = own[keep, s, :, at] if d == 0 else back[u, d - 1, s, :, at]
                    stage[s, d, pl.ds(p, rows, stride=2), :] = banded_dot(x, masks, matrix)
                pieces.at[slot, d].reshape(PAIR, 2 * rows, LEVELS)[s] = stage[s, d].astype(bf16)

        for d in range(n_lev):
            grad_copy(u, d).start()

    mats_copy().start()
    for u in range(PIECES):
        for d in range(n_lev):
            x_copy(u, d).start()
    full_copy().start()
    weight_copy(0).start()
    barrier = greet(n_wave, n_lev)
    mats_copy().wait()
    for b in range(COV_BANDS):
        for a in range(variables):
            mats_t[a, b * LEVELS:(b + 1) * LEVELS, :] = mats[b, a].T
    pl.semaphore_wait(barrier, n_wave + n_lev - 2)
    for d in lev_others:
        table_copy(0, d).start()

    def first(u):
        vertical(u)
        send_levels(u)

    loop(0, AHEAD, first)
    make_order()

    def front(u):
        legendre(u)

        @pl.when(u + AHEAD < units)
        def _():
            vertical(u + AHEAD)
            send_levels(u + AHEAD)

        @pl.when((u >= subs) & (u - subs < lats))
        def _():
            build(u - subs)

    loop(0, units, front)
    loop(0, chunks, grid)

    def last(u):
        @pl.when(u < units)
        def _():
            adjoint_legendre(u)

        @pl.when(u > 0)
        def _():
            adjoint_vertical(u - 1)

    loop(0, units + 1, last)
    inc_copy(chunks - 1).wait()
    for u in range(units - PIECES, units):
        for d in range(n_lev):
            grad_copy(u, d).wait()

    def drain(u):
        for d in lev_others:
            back_copy(units - RING + u, d).wait_send()

    loop(0, RING, drain)


def shards_kernel(n_wave, n_lev, control, wave_of_slot, legendre, vertical, points, lat_band, grid_scale, obs_weight):
    members, slots, rows = control.shape[:3]
    waves = wave_of_slot.shape[0]
    variables = vertical.shape[1]
    columns = control.shape[4]
    cols = columns // n_lev
    lats, _, longs = obs_weight.shape
    chunks = members * variables // n_lev
    subs = slots // PAIR
    units = chunks * subs
    width = 2 * LEVELS
    bf16, f32 = jnp.bfloat16, jnp.float32
    vmem = pl.BlockSpec(memory_space=pltpu.VMEM)
    smem = pl.BlockSpec(memory_space=pltpu.SMEM)
    hbm = pl.BlockSpec(memory_space=pl.ANY)
    dma = pltpu.SemaphoreType.DMA
    others = n_lev - 1
    half = (PAIR, rows, width)
    return pl.pallas_call(
        functools.partial(transform_kernel, n_wave, n_lev),
        out_shape=[
            jax.ShapeDtypeStruct((members, lats, cols, longs), bf16),
            jax.ShapeDtypeStruct(control.shape, bf16),
        ],
        in_specs=[smem, smem, smem, vmem, hbm, hbm, hbm, hbm],
        out_specs=[hbm, hbm],
        scratch_shapes=[
            pltpu.VMEM((n_lev, *legendre.shape), bf16),
            pltpu.VMEM(vertical.shape, bf16),
            pltpu.VMEM((variables, COV_BANDS * LEVELS, LEVELS), bf16),
            pltpu.VMEM((waves, LEVELS), f32),
            pltpu.VMEM((PIECES, n_lev, PAIR, rows, 2, LEVELS), bf16),
            pltpu.VMEM((RING, *half), bf16),
            pltpu.VMEM((RING, others, *half), bf16),
            pltpu.VMEM((units, others, *half), bf16),
            pltpu.VMEM((units, others, *half), bf16),
            pltpu.VMEM((2, n_wave * lats * PAIR, LEVELS), f32),
            pltpu.VMEM((chunks, subs, 2, n_wave, lats, PAIR, LEVELS), bf16),
            pltpu.VMEM((chunks, 2, lats, subs, n_wave, PAIR, LEVELS), bf16),
            pltpu.VMEM((chunks, 2, lats, subs, n_wave, PAIR, LEVELS), bf16),
            pltpu.VMEM((units, 2, n_wave, lats, PAIR, LEVELS), bf16),
            pltpu.VMEM((lats, 2 * waves, longs), bf16),
            pltpu.VMEM((lats, LEVELS, longs), bf16),
            pltpu.VMEM((lats, LEVELS, longs), bf16),
            pltpu.VMEM((PAIR, n_lev, 2 * rows, LEVELS), f32),
            dma, dma, dma((PIECES, n_lev)), dma, dma, dma((PIECES, n_lev)),
            dma((subs, others)), dma((subs, others)),
            dma((units, others)), dma((units, others)), dma((units, others)), dma((units, others)),
            dma((units,)), dma((units,)), dma((units,)), dma((units,)),
        ],
        compiler_params=pltpu.CompilerParams(collective_id=0, has_side_effects=True, vmem_limit_bytes=VMEM_BYTES),
        name="transform",
    )(wave_of_slot, points, lat_band, grid_scale, vertical, control, legendre, obs_weight)


def shards(n_wave, n_lev, *arrays):
    slots, rows, columns = arrays[0].shape[1], arrays[0].shape[2], arrays[0].shape[4]
    whole_tiles = slots % 16 == 0 and rows % 128 == 0 and columns % (n_lev * LEVELS) == 0
    if whole_tiles and n_lev > 1:
        return shards_kernel(n_wave, n_lev, *arrays)
    return shards_plain(*arrays)


def solution(mesh):
    in_specs = (
        P(None, "wave", "lev", None, None),
        P(),
        P("wave", "lev", None),
        P(),
        P("wave"),
        P("wave"),
        P(None, "lev"),
        P("wave", "lev", None),
    )
    out_specs = (P(None, "wave", "lev", None), P(None, "wave", "lev", None, None))
    body = functools.partial(shards, mesh.shape["wave"], mesh.shape["lev"])
    return jax.shard_map(body, mesh=mesh, in_specs=in_specs, out_specs=out_specs, check_vma=False)
```

```python
import functools
import math

import jax
import jax.numpy as jnp
from jax import lax
from jax.experimental import pallas as pl
from jax.experimental.pallas import tpu as pltpu
from jax.sharding import PartitionSpec as P

WAVES = 256
LONGITUDES = 512
LEVELS = 128
VARIABLES = 4
COV_BANDS = 4


def fourier_table(wave_ids, lat_points):
    lon_index = jnp.arange(LONGITUDES, dtype=jnp.int32)
    remainder = wave_ids[None, :, None] * lon_index[None, None, :] % lat_points[:, None, None]
    angles = (
        2.0
        * math.pi
        * remainder.astype(jnp.float32)
        / lat_points.astype(jnp.float32)[:, None, None]
    )
    factor = jnp.where(wave_ids == 0, 1.0, 2.0).astype(jnp.float32) / math.sqrt(4.0 * WAVES)
    inside = lon_index[None, None, :] < lat_points[:, None, None]
    cosine = jnp.where(inside, factor[None, :, None] * jnp.cos(angles), 0.0)
    sine = jnp.where(inside, -factor[None, :, None] * jnp.sin(angles), 0.0)
    return jnp.stack([cosine, sine], axis=2).astype(jnp.bfloat16)


def vertical_apply(field, vertical, live_rows, band_of, forward):
    members, slots, rows_dev = (field.shape[0], field.shape[1], field.shape[2])
    shaped = field.reshape(members, slots, rows_dev, 2, VARIABLES, LEVELS)
    form = "eskpam,alm->eskpal" if forward else "eskpal,alm->eskpam"
    summed = jnp.zeros(shaped.shape, jnp.float32)
    for index_band in range(COV_BANDS):
        partial_value = jnp.einsum(
            form, shaped, vertical[index_band], preferred_element_type=jnp.float32
        )
        chosen = live_rows & (band_of == index_band)
        summed = summed + jnp.where(chosen[None, :, :, None, None, None], partial_value, 0.0)
    return summed.reshape(field.shape).astype(jnp.bfloat16)


def to_bands(values):
    return lax.all_to_all(values, "wave", split_axis=2, concat_axis=1, tiled=True)


def shards_plain(control, wave_of_slot, legendre, vertical, points, lat_band, grid_scale, obs_weight):
    members, slots, rows_dev = (control.shape[0], control.shape[1], control.shape[2])
    slot_start = lax.axis_index("wave") * slots
    row_start = lax.axis_index("lev") * rows_dev
    own_waves = lax.dynamic_slice_in_dim(wave_of_slot, slot_start, slots)
    row_index = row_start + jnp.arange(rows_dev, dtype=jnp.int32)
    totals_n = own_waves[:, None] + row_index[None, :]
    live_rows = totals_n <= WAVES - 1
    band_of = jnp.minimum(totals_n * COV_BANDS // WAVES, COV_BANDS - 1)
    spectral = vertical_apply(control, vertical, live_rows, band_of, True)
    columns = lax.all_to_all(spectral, "lev", split_axis=4, concat_axis=2, tiled=True)
    col_dev = columns.shape[4]
    width = 2 * col_dev
    all_rows = columns.shape[2]
    columns = columns.reshape(members, slots, all_rows, width)
    coeffs = jnp.einsum(
        "skt,eskq->estq",
        lax.all_gather(legendre, "lev", axis=1, tiled=True),
        columns,
        preferred_element_type=jnp.float32,
    )
    coeffs = coeffs.astype(jnp.bfloat16)
    by_lat = to_bands(coeffs)
    wave_count = by_lat.shape[1]
    lat_dev = by_lat.shape[2]
    by_lat = by_lat.reshape(members, wave_count, lat_dev, 2, col_dev)
    fourier = fourier_table(wave_of_slot, points)
    synthesis = jnp.einsum("tspj,estpc->etcj", fourier, by_lat, preferred_element_type=jnp.float32)
    chooser = (
        lat_band[:, None] == jnp.arange(grid_scale.shape[0], dtype=jnp.int32)[None, :]
    ).astype(jnp.float32)
    lat_scale = jnp.dot(chooser, grid_scale, precision=lax.Precision.HIGHEST)
    increment = (synthesis * lat_scale[None, :, :, None]).astype(jnp.bfloat16)
    weighted = (
        increment.astype(jnp.float32) * obs_weight.astype(jnp.float32) * lat_scale[None, :, :, None]
    ).astype(jnp.bfloat16)
    adjoint_fourier = jnp.einsum(
        "tspj,etcj->etspc", fourier, weighted, preferred_element_type=jnp.float32
    )
    adjoint_fourier = adjoint_fourier.astype(jnp.bfloat16).reshape(
        members, lat_dev, wave_count, width
    )
    band_rows = to_bands(adjoint_fourier)
    adjoint_coeffs = jnp.einsum(
        "skt,etsq->eskq",
        lax.all_gather(legendre, "lev", axis=1, tiled=True),
        band_rows,
        preferred_element_type=jnp.float32,
    )
    adjoint_coeffs = adjoint_coeffs.astype(jnp.bfloat16).reshape(
        members, slots, all_rows, 2, col_dev
    )
    rows_back = lax.all_to_all(adjoint_coeffs, "lev", split_axis=2, concat_axis=4, tiled=True)
    gradient = vertical_apply(rows_back, vertical, live_rows, band_of, False)
    return (increment, gradient)


MESH = pl.DeviceIdType.MESH
VMEM_BYTES = 65000 * 1024
PAIR = 2
RING = 8
AHEAD = 4
PIECES = 4


def greet(n_wave, n_lev):
    me_w, me_l = lax.axis_index("wave"), lax.axis_index("lev")
    barrier = pltpu.get_barrier_semaphore()

    def one(d, carry):
        peer = lax.rem(me_w + d, n_wave)
        pl.semaphore_signal(barrier, inc=1, device_id=(peer, me_l), device_id_type=MESH)
        return carry

    lax.fori_loop(1, n_wave, one, 0)
    for d in range(1, n_lev):
        peer = lax.rem(me_l + d, n_lev)
        pl.semaphore_signal(barrier, inc=1, device_id=(me_w, peer), device_id_type=MESH)
    return barrier


def band_masks(total, waves):
    width = waves // COV_BANDS
    masks = []
    for b in range(COV_BANDS):
        hit = (total >= b * width) & (total < (b + 1) * width)
        masks.append(jnp.where(hit, 1.0, 0.0).astype(jnp.bfloat16))
    return masks


def banded_dot(x, masks, matrix):
    stacked = jnp.concatenate([x * mask for mask in masks], axis=1)
    return jnp.dot(stacked, matrix, preferred_element_type=jnp.float32)


SIN_TERMS = [(-1.0) ** i * (2.0 * math.pi) ** (2 * i + 1) / math.factorial(2 * i + 1) for i in range(10)]
COS_TERMS = [(-1.0) ** i * (2.0 * math.pi) ** (2 * i) / math.factorial(2 * i) for i in range(10)]


def horner(terms, square):
    value = jnp.full_like(square, terms[-1])
    for term in terms[-2::-1]:
        value = value * square + term
    return value


def loop(first, last, body):
    def step(i, carry):
        body(i)
        return carry

    lax.fori_loop(first, last, step, 0)


def transform_kernel(n_wave, n_lev, waves_hbm, points_hbm, band_hbm, scale_hbm, v_ref, x_ref, l_ref, weight_ref,
                     inc_ref, grad_ref,
                     waves_ref, points_ref, band_ref, grid_scale_ref, full, mats, mats_t, order, pieces, own, away, spec, back, coef, wsend, asend, land, aland, table, wbuf, ibuf, stage,
                     small_sem, full_sem, mats_sem, x_sem, weight_sem, inc_sem, grad_sem, l_send, l_recv, f_send, f_recv, b_send, b_recv,
                     w_send, w_recv, a_send, a_recv):
    members, slots, rows = x_ref.shape[:3]
    variables = v_ref.shape[1]
    per = variables // n_lev
    lats, cols, longs = weight_ref.shape
    waves = n_wave * slots
    lat_all = n_wave * lats
    chunks = members * per
    subs = slots // PAIR
    units = chunks * subs
    me_w, me_l = lax.axis_index("wave"), lax.axis_index("lev")
    row0 = me_l * rows
    bf16, f32 = jnp.bfloat16, jnp.float32

    def where_is(u):
        q, g = lax.div(u, subs), lax.rem(u, subs)
        return q, g, lax.div(q, per), lax.rem(q, per)

    def level_block(d, i):
        a = lax.rem(me_l + d, n_lev) * per + i
        return a, pl.ds(pl.multiple_of(a * LEVELS, LEVELS), LEVELS)

    def pair_slots(g):
        return pl.ds(g * PAIR, PAIR)

    def x_copy(u, d):
        _, g, e, i = where_is(u)
        slot = lax.rem(u, PIECES)
        return pltpu.make_async_copy(
            x_ref.at[e, pair_slots(g), :, :, level_block(d, i)[1]], pieces.at[slot, d], x_sem.at[slot, d])

    def grad_copy(u, d):
        _, g, e, i = where_is(u)
        slot = lax.rem(u, PIECES)
        return pltpu.make_async_copy(
            pieces.at[slot, d], grad_ref.at[e, pair_slots(g), :, :, level_block(d, i)[1]], grad_sem.at[slot, d])

    def weight_copy(q):
        i = lax.rem(q, per)
        return pltpu.make_async_copy(
            weight_ref.at[:, pl.ds(pl.multiple_of(i * LEVELS, LEVELS), LEVELS), :], wbuf, weight_sem)

    def inc_copy(q):
        e, i = lax.div(q, per), lax.rem(q, per)
        return pltpu.make_async_copy(
            ibuf, inc_ref.at[e, :, pl.ds(pl.multiple_of(i * LEVELS, LEVELS), LEVELS), :], inc_sem)

    def full_copy():
        return pltpu.make_async_copy(l_ref, full.at[me_l], full_sem)

    def small_copies():
        pairs = [(waves_hbm, waves_ref), (scale_hbm, grid_scale_ref), (points_hbm, points_ref), (band_hbm, band_ref)]
        return [pltpu.make_async_copy(src, dst, small_sem.at[k]) for k, (src, dst) in enumerate(pairs)]

    def mats_copy():
        return pltpu.make_async_copy(v_ref, mats, mats_sem)

    def table_copy(g, d):
        peer = lax.rem(me_l + d, n_lev)
        return pltpu.make_async_remote_copy(
            src_ref=l_ref.at[pair_slots(g)], dst_ref=full.at[me_l, pair_slots(g)],
            send_sem=l_send.at[g, d - 1], recv_sem=l_recv.at[g, d - 1],
            device_id=(me_w, peer), device_id_type=MESH)

    def lev_copy(u, d, target, send_sem, recv_sem):
        peer = lax.rem(me_l + d, n_lev)
        return pltpu.make_async_remote_copy(
            src_ref=away.at[lax.rem(u, RING), d - 1], dst_ref=target.at[u, n_lev - d - 1],
            send_sem=send_sem.at[u, d - 1], recv_sem=recv_sem.at[u, d - 1],
            device_id=(me_w, peer), device_id_type=MESH)

    def out_copy(u, d):
        return lev_copy(u, d, spec, f_send, f_recv)

    def back_copy(u, d):
        return lev_copy(u, d, back, b_send, b_recv)

    def remote(src, dst, send_sem, recv_sem, d):
        return pltpu.make_async_remote_copy(
            src_ref=src, dst_ref=dst, send_sem=send_sem, recv_sem=recv_sem,
            device_id=(lax.rem(me_w + d, n_wave), me_l), device_id_type=MESH)

    def land_copy(u, d):
        q, g, _, _ = where_is(u)
        peer = lax.rem(me_w + d, n_wave)
        return remote(wsend.at[q, g, :, peer], land.at[q, :, :, g, me_w], w_send.at[u], w_recv.at[u], d)

    def land_all(u):
        q, g, _, _ = where_is(u)
        most = pl.ds(0, n_wave - 1)
        return remote(wsend.at[q, g, :, most], land.at[q, :, :, g, most], w_send.at[u], w_recv.at[u], 1)

    def aland_copy(u, d):
        q, g, _, _ = where_is(u)
        peer = lax.rem(me_w + d, n_wave)
        return remote(asend.at[q, :, :, g, peer], aland.at[u, :, me_w], a_send.at[u], a_recv.at[u], d)

    def aland_all(u):
        q, g, _, _ = where_is(u)
        most = pl.ds(0, n_wave - 1)
        return remote(asend.at[q, :, :, g, most], aland.at[u, :, most], a_send.at[u], a_recv.at[u], 1)

    lev_others = range(1, n_lev)
    lev_order = list(lev_others) + [0]

    def own_wave(g, s):
        return waves_ref[me_w * slots + g * PAIR + s]

    def vertical(u):
        _, g, e, i = where_is(u)
        slot, keep = lax.rem(u, PIECES), lax.rem(u, RING)
        for d in range(n_lev):
            x_copy(u, d).wait()

        @pl.when(u >= RING)
        def _():
            for d in lev_others:
                out_copy(u - RING, d).wait_send()

        for s in range(PAIR):
            total = own_wave(g, s) + row0 + lax.div(lax.broadcasted_iota(jnp.int32, (2 * rows, LEVELS), 0), 2)
            masks = band_masks(total, waves)
            for d in lev_order:
                a, _ = level_block(d, i)
                x = pieces.at[slot, d].reshape(PAIR, 2 * rows, LEVELS)[s]
                stage[s, d] = banded_dot(x, masks, mats_t[a])
                for p in range(2):
                    y = stage[s, d, pl.ds(p, rows, stride=2), :].astype(bf16)
                    if d == 0:
                        own[keep, s, :, p * LEVELS:(p + 1) * LEVELS] = y
                    else:
                        away[keep, d - 1, s, :, p * LEVELS:(p + 1) * LEVELS] = y

        @pl.when(u + PIECES < units)
        def _():
            for d in range(n_lev):
                x_copy(u + PIECES, d).start()

    def send_levels(u):
        for d in lev_others:
            out_copy(u, d).start()

        @pl.when(u + 1 < subs)
        def _():
            for d in lev_others:
                table_copy(u + 1, d).start()

    def legendre(u):
        q, g, e, i = where_is(u)
        keep = lax.rem(u, RING)

        @pl.when(u == 0)
        def _():
            full_copy().wait()

        @pl.when(u < subs)
        def _():
            for d in lev_others:
                table_copy(u, d).wait()

        for d in lev_others:
            out_copy(u, d).wait_recv()

        for s in range(PAIR):
            fields, tables = [], []
            for d in range(n_lev):
                fields.append(own[keep, s] if d == 0 else spec[u, d - 1, s])
                tables.append(full[lax.rem(me_l + d, n_lev), g * PAIR + s])
            value = lax.dot_general(
                jnp.concatenate(tables, axis=0), jnp.concatenate(fields, axis=0),
                (((0,), (0,)), ((), ())), preferred_element_type=f32)
            for p in range(2):
                coef[p, pl.ds(s, lat_all, stride=PAIR), :] = value[:, p * LEVELS:(p + 1) * LEVELS]
        for p in range(2):
            wsend.at[q, g, p].reshape(lat_all * PAIR, LEVELS)[...] = coef[p].astype(bf16)
        loop(1, n_wave, lambda d: land_copy(u, d).start())
        land[q, :, :, g, me_w] = wsend[q, g, :, me_w]

    def make_order():
        def some(k):
            row = lax.broadcasted_iota(jnp.int32, (8, LEVELS), 0)
            values = jnp.zeros((8, LEVELS), jnp.int32)
            for j in range(8):
                r = k * 8 + j
                g, w, s = lax.div(r, n_wave * PAIR), lax.rem(lax.div(r, PAIR), n_wave), lax.rem(r, PAIR)
                values = jnp.where(row == j, waves_ref[w * slots + g * PAIR + s], values)
            order[pl.ds(pl.multiple_of(k * 8, 8), 8), :] = values.astype(f32)

        loop(0, waves // 8, some)

    def build(t):
        points = points_ref[t]
        n = points.astype(f32)
        piece = 32
        inverse = 1.0 / jnp.full((1, longs), n, f32)
        lane = lax.broadcasted_iota(jnp.int32, (1, longs), 1)
        inside = jnp.where(lane < points, 1.0, 0.0) / math.sqrt(4.0 * waves)

        def some(k):
            base = pl.multiple_of(k * piece, piece)
            wave = order[pl.ds(base, piece), 0:1]
            product = wave * lane.astype(f32)
            turns = jnp.floor(product * inverse + 0.5)
            x = (product - turns * n) * inverse
            square = x * x
            gain = jnp.where(wave == 0.0, 1.0, 2.0) * inside
            table[t, pl.ds(base, piece), :] = (gain * horner(COS_TERMS, square)).astype(bf16)
            sine = (-gain) * (x * horner(SIN_TERMS, square))
            table[t, pl.ds(pl.multiple_of(waves + base, piece), piece), :] = sine.astype(bf16)

        loop(0, waves // piece, some)

    def scale_column(t, i):
        block = grid_scale_ref[:, pl.ds(pl.multiple_of(i * LEVELS, LEVELS), LEVELS)]
        band = lax.broadcasted_iota(jnp.int32, block.shape, 0)
        line = jnp.sum(jnp.where(band == band_ref[t], block, 0.0), axis=0, keepdims=True)
        square = (LEVELS, LEVELS)
        diagonal = lax.broadcasted_iota(jnp.int32, square, 0) == lax.broadcasted_iota(jnp.int32, square, 1)
        return jnp.sum(jnp.where(diagonal, line, 0.0), axis=1, keepdims=True)

    def grid(q):
        i = lax.rem(q, per)
        weight_copy(q).wait()

        @pl.when(q > 0)
        def _():
            inc_copy(q - 1).wait()

        loop(0, subs, lambda g: land_all(q * subs + g).wait())

        def one(t):
            scale = scale_column(t, i)
            parts = [land.at[q, p, t].reshape(waves, LEVELS)[...] for p in range(2)]
            synthesis = lax.dot_general(jnp.concatenate(parts, axis=0), table[t], (((0,), (0,)), ((), ())),
                                        preferred_element_type=f32)
            increment = (synthesis * scale).astype(bf16)
            ibuf[t] = increment
            weighted = increment.astype(f32) * wbuf[t].astype(f32) * scale
            adjoint = lax.dot_general(table[t], weighted.astype(bf16), (((1,), (1,)), ((), ())),
                                      preferred_element_type=f32).astype(bf16)
            for p in range(2):
                asend.at[q, p, t].reshape(waves, LEVELS)[...] = adjoint[p * waves:(p + 1) * waves]

        loop(0, lats, one)

        def send(g):
            u = q * subs + g
            loop(1, n_wave, lambda d: aland_copy(u, d).start())
            aland[u, :, me_w] = asend[q, :, :, g, me_w]

        loop(0, subs, send)
        inc_copy(q).start()

        @pl.when(q + 1 < chunks)
        def _():
            weight_copy(q + 1).start()

    def project(d, g, s, field):
        table_part = full[lax.rem(me_l + d, n_lev), g * PAIR + s]
        return jnp.dot(table_part, field, preferred_element_type=f32).astype(bf16)

    def adjoint_legendre(u):
        _, g, e, i = where_is(u)
        keep = lax.rem(u, RING)
        aland_all(u).wait()

        @pl.when(u < RING)
        def _():
            for d in lev_others:
                out_copy(u + units - RING, d).wait_send()

        @pl.when(u >= RING)
        def _():
            for d in lev_others:
                back_copy(u - RING, d).wait_send()

        for p in range(2):
            coef[p] = aland.at[u, p].reshape(lat_all * PAIR, LEVELS)[...].astype(f32)
        fields = []
        for s in range(PAIR):
            field = jnp.concatenate(
                [coef[p, pl.ds(s, lat_all, stride=PAIR), :].astype(bf16) for p in range(2)], axis=1)
            fields.append(field)
            for d in lev_others:
                away[keep, d - 1, s] = project(d, g, s, field)
        for d in lev_others:
            back_copy(u, d).start()
        for s in range(PAIR):
            own[keep, s] = project(0, g, s, fields[s])

    def adjoint_vertical(u):
        _, g, e, i = where_is(u)
        slot, keep = lax.rem(u, PIECES), lax.rem(u, RING)
        @pl.when(u >= PIECES)
        def _():
            for d in range(n_lev):
                grad_copy(u - PIECES, d).wait()

        masks = [
            band_masks(own_wave(g, s) + row0 + lax.broadcasted_iota(jnp.int32, (rows, LEVELS), 0), waves)
            for s in range(PAIR)
        ]
        for d in range(n_lev):
            if d > 0:
                back_copy(u, d).wait_recv()
            a, _ = level_block(d, i)
            matrix = mats[:, a].reshape(COV_BANDS * LEVELS, LEVELS)
            for s in range(PAIR):
                for p in range(2):
                    at = slice(p * LEVELS, (p + 1) * LEVELS)
                    x = own[keep, s, :, at] if d == 0 else back[u, d - 1, s, :, at]
                    stage[s, d, pl.ds(p, rows, stride=2), :] = banded_dot(x, masks[s], matrix)
                pieces.at[slot, d].reshape(PAIR, 2 * rows, LEVELS)[s] = stage[s, d].astype(bf16)
            grad_copy(u, d).start()

    for copy in small_copies():
        copy.start()
    mats_copy().start()
    for u in range(PIECES):
        for d in range(n_lev):
            x_copy(u, d).start()
    full_copy().start()
    weight_copy(0).start()
    barrier = greet(n_wave, n_lev)
    mats_copy().wait()
    for b in range(COV_BANDS):
        for a in range(variables):
            mats_t[a, b * LEVELS:(b + 1) * LEVELS, :] = mats[b, a].T
    for copy in small_copies():
        copy.wait()
    pl.semaphore_wait(barrier, n_wave + n_lev - 2)
    for d in lev_others:
        table_copy(0, d).start()

    def first(u):
        vertical(u)
        send_levels(u)

    loop(0, AHEAD, first)

    def front(u):
        legendre(u)

        @pl.when(u + AHEAD < units)
        def _():
            vertical(u + AHEAD)
            send_levels(u + AHEAD)

        @pl.when(u == subs - 1)
        def _():
            make_order()

        @pl.when((u >= subs) & (u - subs < lats))
        def _():
            build(u - subs)

    loop(0, units, front)
    loop(0, chunks, grid)

    def last(u):
        @pl.when(u < units)
        def _():
            adjoint_legendre(u)

        @pl.when(u > 0)
        def _():
            adjoint_vertical(u - 1)

    loop(0, units + 1, last)
    inc_copy(chunks - 1).wait()
    for u in range(units - PIECES, units):
        for d in range(n_lev):
            grad_copy(u, d).wait()

    def drain(u):
        for d in lev_others:
            back_copy(units - RING + u, d).wait_send()

    loop(0, RING, drain)


def settle_kernel(inc_ref, grad_ref, inc_out, grad_out, a, b, a_in, a_out, b_in, b_out):
    def moves(i):
        return [
            (pltpu.make_async_copy(inc_ref.at[:, i], a.at[i], a_in.at[i]),
             pltpu.make_async_copy(a.at[i], inc_out.at[:, i], a_out.at[i])),
            (pltpu.make_async_copy(grad_ref.at[:, i], b.at[i], b_in.at[i]),
             pltpu.make_async_copy(b.at[i], grad_out.at[:, i], b_out.at[i])),
        ]

    steps = a.shape[0]
    stages = [moves(i) for i in range(steps)]
    for pairs in stages:
        for first, _ in pairs:
            first.start()
    for pairs in stages:
        for first, then in pairs:
            first.wait()
            then.start()
    for pairs in stages:
        for _, then in pairs:
            then.wait()


def settle(increment, gradient):
    hbm = pl.BlockSpec(memory_space=pl.ANY)
    dma = pltpu.SemaphoreType.DMA
    shapes = [increment.shape, gradient.shape]
    steps = increment.shape[1]
    kept = [pltpu.VMEM((steps, s[0], *s[2:]), jnp.bfloat16) for s in shapes]
    return pl.pallas_call(
        settle_kernel,
        out_shape=[jax.ShapeDtypeStruct(s, jnp.bfloat16) for s in shapes],
        in_specs=[hbm, hbm],
        out_specs=[hbm, hbm],
        scratch_shapes=[*kept, *[dma((steps,))] * 4],
        compiler_params=pltpu.CompilerParams(vmem_limit_bytes=VMEM_BYTES),
        name="settle",
    )(increment, gradient)


def shards_kernel(n_wave, n_lev, control, wave_of_slot, legendre, vertical, points, lat_band, grid_scale, obs_weight):
    members, slots, rows = control.shape[:3]
    waves = wave_of_slot.shape[0]
    variables = vertical.shape[1]
    columns = control.shape[4]
    cols = columns // n_lev
    lats, _, longs = obs_weight.shape
    chunks = members * variables // n_lev
    subs = slots // PAIR
    units = chunks * subs
    width = 2 * LEVELS
    bf16, f32 = jnp.bfloat16, jnp.float32
    hbm = pl.BlockSpec(memory_space=pl.ANY)
    dma = pltpu.SemaphoreType.DMA
    others = n_lev - 1
    half = (PAIR, rows, width)
    results = pl.pallas_call(
        functools.partial(transform_kernel, n_wave, n_lev),
        out_shape=[
            jax.ShapeDtypeStruct((members, lats, cols, longs), bf16),
            jax.ShapeDtypeStruct(control.shape, bf16),
        ],
        in_specs=[hbm] * 8,
        out_specs=[hbm, hbm],
        scratch_shapes=[
            pltpu.SMEM(wave_of_slot.shape, jnp.int32),
            pltpu.SMEM(points.shape, jnp.int32),
            pltpu.SMEM(lat_band.shape, jnp.int32),
            pltpu.VMEM(grid_scale.shape, f32),
            pltpu.VMEM((n_lev, *legendre.shape), bf16),
            pltpu.VMEM(vertical.shape, bf16),
            pltpu.VMEM((variables, COV_BANDS * LEVELS, LEVELS), bf16),
            pltpu.VMEM((waves, LEVELS), f32),
            pltpu.VMEM((PIECES, n_lev, PAIR, rows, 2, LEVELS), bf16),
            pltpu.VMEM((RING, *half), bf16),
            pltpu.VMEM((RING, others, *half), bf16),
            pltpu.VMEM((units, others, *half), bf16),
            pltpu.VMEM((units, others, *half), bf16),
            pltpu.VMEM((2, n_wave * lats * PAIR, LEVELS), f32),
            pltpu.VMEM((chunks, subs, 2, n_wave, lats, PAIR, LEVELS), bf16),
            pltpu.VMEM((chunks, 2, lats, subs, n_wave, PAIR, LEVELS), bf16),
            pltpu.VMEM((chunks, 2, lats, subs, n_wave, PAIR, LEVELS), bf16),
            pltpu.VMEM((units, 2, n_wave, lats, PAIR, LEVELS), bf16),
            pltpu.VMEM((lats, 2 * waves, longs), bf16),
            pltpu.VMEM((lats, LEVELS, longs), bf16),
            pltpu.VMEM((lats, LEVELS, longs), bf16),
            pltpu.VMEM((PAIR, n_lev, 2 * rows, LEVELS), f32),
            dma((4,)), dma, dma, dma((PIECES, n_lev)), dma, dma, dma((PIECES, n_lev)),
            dma((subs, others)), dma((subs, others)),
            dma((units, others)), dma((units, others)), dma((units, others)), dma((units, others)),
            dma((units,)), dma((units,)), dma((units,)), dma((units,)),
        ],
        compiler_params=pltpu.CompilerParams(collective_id=0, has_side_effects=True, vmem_limit_bytes=VMEM_BYTES),
        name="transform",
    )(wave_of_slot, points, lat_band, grid_scale, vertical, control, legendre, obs_weight)
    return tuple(settle(*results))


def shards(n_wave, n_lev, *arrays):
    slots, rows, columns = arrays[0].shape[1], arrays[0].shape[2], arrays[0].shape[4]
    whole_tiles = slots % 16 == 0 and rows % 128 == 0 and columns % (n_lev * LEVELS) == 0
    if whole_tiles and n_lev > 1:
        return shards_kernel(n_wave, n_lev, *arrays)
    return shards_plain(*arrays)


def solution(mesh):
    in_specs = (
        P(None, "wave", "lev", None, None),
        P(),
        P("wave", "lev", None),
        P(),
        P("wave"),
        P("wave"),
        P(None, "lev"),
        P("wave", "lev", None),
    )
    out_specs = (P(None, "wave", "lev", None), P(None, "wave", "lev", None, None))
    body = functools.partial(shards, mesh.shape["wave"], mesh.shape["lev"])
    return jax.shard_map(body, mesh=mesh, in_specs=in_specs, out_specs=out_specs, check_vma=False)
```

```python
import functools
import math

import jax
import jax.numpy as jnp
from jax import lax
from jax.experimental import pallas as pl
from jax.experimental.pallas import tpu as pltpu
from jax.sharding import PartitionSpec as P

WAVES = 256
LONGITUDES = 512
LEVELS = 128
VARIABLES = 4
COV_BANDS = 4


def fourier_table(wave_ids, lat_points):
    lon_index = jnp.arange(LONGITUDES, dtype=jnp.int32)
    remainder = wave_ids[None, :, None] * lon_index[None, None, :] % lat_points[:, None, None]
    angles = (
        2.0
        * math.pi
        * remainder.astype(jnp.float32)
        / lat_points.astype(jnp.float32)[:, None, None]
    )
    factor = jnp.where(wave_ids == 0, 1.0, 2.0).astype(jnp.float32) / math.sqrt(4.0 * WAVES)
    inside = lon_index[None, None, :] < lat_points[:, None, None]
    cosine = jnp.where(inside, factor[None, :, None] * jnp.cos(angles), 0.0)
    sine = jnp.where(inside, -factor[None, :, None] * jnp.sin(angles), 0.0)
    return jnp.stack([cosine, sine], axis=2).astype(jnp.bfloat16)


def vertical_apply(field, vertical, live_rows, band_of, forward):
    members, slots, rows_dev = (field.shape[0], field.shape[1], field.shape[2])
    shaped = field.reshape(members, slots, rows_dev, 2, VARIABLES, LEVELS)
    form = "eskpam,alm->eskpal" if forward else "eskpal,alm->eskpam"
    summed = jnp.zeros(shaped.shape, jnp.float32)
    for index_band in range(COV_BANDS):
        partial_value = jnp.einsum(
            form, shaped, vertical[index_band], preferred_element_type=jnp.float32
        )
        chosen = live_rows & (band_of == index_band)
        summed = summed + jnp.where(chosen[None, :, :, None, None, None], partial_value, 0.0)
    return summed.reshape(field.shape).astype(jnp.bfloat16)


def to_bands(values):
    return lax.all_to_all(values, "wave", split_axis=2, concat_axis=1, tiled=True)


def shards_plain(control, wave_of_slot, legendre, vertical, points, lat_band, grid_scale, obs_weight):
    members, slots, rows_dev = (control.shape[0], control.shape[1], control.shape[2])
    slot_start = lax.axis_index("wave") * slots
    row_start = lax.axis_index("lev") * rows_dev
    own_waves = lax.dynamic_slice_in_dim(wave_of_slot, slot_start, slots)
    row_index = row_start + jnp.arange(rows_dev, dtype=jnp.int32)
    totals_n = own_waves[:, None] + row_index[None, :]
    live_rows = totals_n <= WAVES - 1
    band_of = jnp.minimum(totals_n * COV_BANDS // WAVES, COV_BANDS - 1)
    spectral = vertical_apply(control, vertical, live_rows, band_of, True)
    columns = lax.all_to_all(spectral, "lev", split_axis=4, concat_axis=2, tiled=True)
    col_dev = columns.shape[4]
    width = 2 * col_dev
    all_rows = columns.shape[2]
    columns = columns.reshape(members, slots, all_rows, width)
    coeffs = jnp.einsum(
        "skt,eskq->estq",
        lax.all_gather(legendre, "lev", axis=1, tiled=True),
        columns,
        preferred_element_type=jnp.float32,
    )
    coeffs = coeffs.astype(jnp.bfloat16)
    by_lat = to_bands(coeffs)
    wave_count = by_lat.shape[1]
    lat_dev = by_lat.shape[2]
    by_lat = by_lat.reshape(members, wave_count, lat_dev, 2, col_dev)
    fourier = fourier_table(wave_of_slot, points)
    synthesis = jnp.einsum("tspj,estpc->etcj", fourier, by_lat, preferred_element_type=jnp.float32)
    chooser = (
        lat_band[:, None] == jnp.arange(grid_scale.shape[0], dtype=jnp.int32)[None, :]
    ).astype(jnp.float32)
    lat_scale = jnp.dot(chooser, grid_scale, precision=lax.Precision.HIGHEST)
    increment = (synthesis * lat_scale[None, :, :, None]).astype(jnp.bfloat16)
    weighted = (
        increment.astype(jnp.float32) * obs_weight.astype(jnp.float32) * lat_scale[None, :, :, None]
    ).astype(jnp.bfloat16)
    adjoint_fourier = jnp.einsum(
        "tspj,etcj->etspc", fourier, weighted, preferred_element_type=jnp.float32
    )
    adjoint_fourier = adjoint_fourier.astype(jnp.bfloat16).reshape(
        members, lat_dev, wave_count, width
    )
    band_rows = to_bands(adjoint_fourier)
    adjoint_coeffs = jnp.einsum(
        "skt,etsq->eskq",
        lax.all_gather(legendre, "lev", axis=1, tiled=True),
        band_rows,
        preferred_element_type=jnp.float32,
    )
    adjoint_coeffs = adjoint_coeffs.astype(jnp.bfloat16).reshape(
        members, slots, all_rows, 2, col_dev
    )
    rows_back = lax.all_to_all(adjoint_coeffs, "lev", split_axis=2, concat_axis=4, tiled=True)
    gradient = vertical_apply(rows_back, vertical, live_rows, band_of, False)
    return (increment, gradient)


MESH = pl.DeviceIdType.MESH
VMEM_BYTES = 65000 * 1024
PAIR = 2
RING = 8
AHEAD = 4
PIECES = 4


def greet(n_wave, n_lev):
    me_w, me_l = lax.axis_index("wave"), lax.axis_index("lev")
    barrier = pltpu.get_barrier_semaphore()

    def one(d, carry):
        peer = lax.rem(me_w + d, n_wave)
        pl.semaphore_signal(barrier, inc=1, device_id=(peer, me_l), device_id_type=MESH)
        return carry

    lax.fori_loop(1, n_wave, one, 0)
    for d in range(1, n_lev):
        peer = lax.rem(me_l + d, n_lev)
        pl.semaphore_signal(barrier, inc=1, device_id=(me_w, peer), device_id_type=MESH)
    return barrier


def band_masks(total, waves):
    width = waves // COV_BANDS
    masks = []
    for b in range(COV_BANDS):
        hit = (total >= b * width) & (total < (b + 1) * width)
        masks.append(jnp.where(hit, 1.0, 0.0).astype(jnp.bfloat16))
    return masks


def banded_dot(x, masks, matrix):
    stacked = jnp.concatenate([x * mask for mask in masks], axis=1)
    return jnp.dot(stacked, matrix, preferred_element_type=jnp.float32)


SIN_TERMS = [(-1.0) ** i * (2.0 * math.pi) ** (2 * i + 1) / math.factorial(2 * i + 1) for i in range(10)]
COS_TERMS = [(-1.0) ** i * (2.0 * math.pi) ** (2 * i) / math.factorial(2 * i) for i in range(10)]


def horner(terms, square):
    value = jnp.full_like(square, terms[-1])
    for term in terms[-2::-1]:
        value = value * square + term
    return value


def loop(first, last, body):
    def step(i, carry):
        body(i)
        return carry

    lax.fori_loop(first, last, step, 0)


def transform_kernel(n_wave, n_lev, waves_hbm, points_hbm, band_hbm, scale_hbm, v_ref, x_ref, l_ref, weight_ref,
                     inc_ref, grad_ref,
                     waves_ref, points_ref, band_ref, grid_scale_ref, full, mats, mats_t, order, pieces, own, away, spec, back, coef, wsend, asend, land, aland, table, wbuf, ibuf, stage,
                     small_sem, full_sem, mats_sem, x_sem, weight_sem, inc_sem, grad_sem, l_send, l_recv, f_send, f_recv, b_send, b_recv,
                     w_send, w_recv, a_send, a_recv):
    members, slots, rows = x_ref.shape[:3]
    variables = v_ref.shape[1]
    per = variables // n_lev
    lats, cols, longs = weight_ref.shape
    waves = n_wave * slots
    lat_all = n_wave * lats
    chunks = members * per
    subs = slots // PAIR
    units = chunks * subs
    me_w, me_l = lax.axis_index("wave"), lax.axis_index("lev")
    row0 = me_l * rows
    bf16, f32 = jnp.bfloat16, jnp.float32

    def where_is(u):
        q, g = lax.div(u, subs), lax.rem(u, subs)
        return q, g, lax.div(q, per), lax.rem(q, per)

    def level_block(d, i):
        a = lax.rem(me_l + d, n_lev) * per + i
        return a, pl.ds(pl.multiple_of(a * LEVELS, LEVELS), LEVELS)

    def pair_slots(g):
        return pl.ds(g * PAIR, PAIR)

    def x_copy(u, d):
        _, g, e, i = where_is(u)
        slot = lax.rem(u, PIECES)
        return pltpu.make_async_copy(
            x_ref.at[e, pair_slots(g), :, :, level_block(d, i)[1]], pieces.at[slot, d], x_sem.at[slot, d])

    def grad_copy(u, d):
        _, g, e, i = where_is(u)
        slot = lax.rem(u, PIECES)
        return pltpu.make_async_copy(
            pieces.at[slot, d], grad_ref.at[e, pair_slots(g), :, :, level_block(d, i)[1]], grad_sem.at[slot, d])

    def weight_copy(q):
        i = lax.rem(q, per)
        return pltpu.make_async_copy(
            weight_ref.at[:, pl.ds(pl.multiple_of(i * LEVELS, LEVELS), LEVELS), :], wbuf, weight_sem)

    def inc_copy(q):
        e, i = lax.div(q, per), lax.rem(q, per)
        return pltpu.make_async_copy(
            ibuf, inc_ref.at[e, :, pl.ds(pl.multiple_of(i * LEVELS, LEVELS), LEVELS), :], inc_sem)

    def full_copy():
        return pltpu.make_async_copy(l_ref, full.at[me_l], full_sem)

    def small_copies():
        pairs = [(waves_hbm, waves_ref), (scale_hbm, grid_scale_ref), (points_hbm, points_ref), (band_hbm, band_ref)]
        return [pltpu.make_async_copy(src, dst, small_sem.at[k]) for k, (src, dst) in enumerate(pairs)]

    def mats_copy():
        return pltpu.make_async_copy(v_ref, mats, mats_sem)

    def table_copy(g, d):
        peer = lax.rem(me_l + d, n_lev)
        return pltpu.make_async_remote_copy(
            src_ref=l_ref.at[pair_slots(g)], dst_ref=full.at[me_l, pair_slots(g)],
            send_sem=l_send.at[g, d - 1], recv_sem=l_recv.at[g, d - 1],
            device_id=(me_w, peer), device_id_type=MESH)

    def lev_copy(u, d, p, target, send_sem, recv_sem):
        peer = lax.rem(me_l + d, n_lev)
        at = pl.ds(p * LEVELS, LEVELS)
        return pltpu.make_async_remote_copy(
            src_ref=away.at[lax.rem(u, RING), d - 1, :, :, at], dst_ref=target.at[u, n_lev - d - 1, :, :, at],
            send_sem=send_sem.at[u, d - 1, p], recv_sem=recv_sem.at[u, d - 1, p],
            device_id=(me_w, peer), device_id_type=MESH)

    def out_copy(u, d, p):
        return lev_copy(u, d, p, spec, f_send, f_recv)

    def back_copy(u, d, p):
        return lev_copy(u, d, p, back, b_send, b_recv)

    lev_parts = [(d, p) for p in range(2) for d in range(1, n_lev)]

    def remote(src, dst, send_sem, recv_sem, d):
        return pltpu.make_async_remote_copy(
            src_ref=src, dst_ref=dst, send_sem=send_sem, recv_sem=recv_sem,
            device_id=(lax.rem(me_w + d, n_wave), me_l), device_id_type=MESH)

    def land_copy(u, d):
        q, g, _, _ = where_is(u)
        peer = lax.rem(me_w + d, n_wave)
        return remote(wsend.at[q, g, :, peer], land.at[q, :, :, g, me_w], w_send.at[u], w_recv.at[u], d)

    def land_all(u):
        q, g, _, _ = where_is(u)
        most = pl.ds(0, n_wave - 1)
        return remote(wsend.at[q, g, :, most], land.at[q, :, :, g, most], w_send.at[u], w_recv.at[u], 1)

    def land_half(u, p, d):
        q, g, _, _ = where_is(u)
        peer = lax.rem(me_w + d, n_wave)
        return remote(wsend.at[q, g, p, peer], land.at[q, p, :, g, me_w], w_send.at[u], w_recv.at[u], d)

    def aland_half(p, d):
        peer = lax.rem(me_w + d, n_wave)
        return remote(asend.at[chunks - 1, p, :, subs - 1, peer], aland.at[units - 1, p, me_w],
                      a_send.at[units - 1 + p], a_recv.at[units - 1 + p], d)

    def aland_half_all(p):
        most = pl.ds(0, n_wave - 1)
        return remote(asend.at[chunks - 1, p, :, subs - 1, most], aland.at[units - 1, p, most],
                      a_send.at[units - 1 + p], a_recv.at[units - 1 + p], 1)

    def aland_copy(u, d):
        q, g, _, _ = where_is(u)
        peer = lax.rem(me_w + d, n_wave)
        return remote(asend.at[q, :, :, g, peer], aland.at[u, :, me_w], a_send.at[u], a_recv.at[u], d)

    def aland_all(u):
        q, g, _, _ = where_is(u)
        most = pl.ds(0, n_wave - 1)
        return remote(asend.at[q, :, :, g, most], aland.at[u, :, most], a_send.at[u], a_recv.at[u], 1)

    lev_others = range(1, n_lev)
    lev_order = list(lev_others) + [0]

    def own_wave(g, s):
        return waves_ref[me_w * slots + g * PAIR + s]

    def vertical(u):
        _, g, e, i = where_is(u)
        slot, keep = lax.rem(u, PIECES), lax.rem(u, RING)
        for d in range(n_lev):
            x_copy(u, d).wait()

        @pl.when(u >= RING)
        def _():
            for d, p in lev_parts:
                out_copy(u - RING, d, p).wait_send()

        for s in range(PAIR):
            total = own_wave(g, s) + row0 + lax.div(lax.broadcasted_iota(jnp.int32, (2 * rows, LEVELS), 0), 2)
            masks = band_masks(total, waves)
            for d in lev_order:
                a, _ = level_block(d, i)
                x = pieces.at[slot, d].reshape(PAIR, 2 * rows, LEVELS)[s]
                stage[s, d] = banded_dot(x, masks, mats_t[a])
                for p in range(2):
                    y = stage[s, d, pl.ds(p, rows, stride=2), :].astype(bf16)
                    if d == 0:
                        own[keep, s, :, p * LEVELS:(p + 1) * LEVELS] = y
                    else:
                        away[keep, d - 1, s, :, p * LEVELS:(p + 1) * LEVELS] = y

        @pl.when(u + PIECES < units)
        def _():
            for d in range(n_lev):
                x_copy(u + PIECES, d).start()

    def send_levels(u):
        for d, p in lev_parts:
            out_copy(u, d, p).start()

        @pl.when(u + 1 < subs)
        def _():
            for d in lev_others:
                table_copy(u + 1, d).start()

    def legendre(u):
        q, g, e, i = where_is(u)
        keep = lax.rem(u, RING)

        @pl.when(u == 0)
        def _():
            full_copy().wait()

        @pl.when(u < subs)
        def _():
            for d in lev_others:
                table_copy(u, d).wait()

        for p in range(2):
            at = slice(p * LEVELS, (p + 1) * LEVELS)
            for d in lev_others:
                out_copy(u, d, p).wait_recv()
            for s in range(PAIR):
                fields, tables = [], []
                for d in range(n_lev):
                    fields.append(own[keep, s, :, at] if d == 0 else spec[u, d - 1, s, :, at])
                    tables.append(full[lax.rem(me_l + d, n_lev), g * PAIR + s])
                coef[p, pl.ds(s, lat_all, stride=PAIR), :] = lax.dot_general(
                    jnp.concatenate(tables, axis=0), jnp.concatenate(fields, axis=0),
                    (((0,), (0,)), ((), ())), preferred_element_type=f32)
            wsend.at[q, g, p].reshape(lat_all * PAIR, LEVELS)[...] = coef[p].astype(bf16)

            @pl.when(u == 0)
            def _():
                loop(1, n_wave, lambda d: land_half(u, p, d).start())

        @pl.when(u > 0)
        def _():
            loop(1, n_wave, lambda d: land_copy(u, d).start())

        land[q, :, :, g, me_w] = wsend[q, g, :, me_w]

    def make_order():
        def some(k):
            row = lax.broadcasted_iota(jnp.int32, (8, LEVELS), 0)
            values = jnp.zeros((8, LEVELS), jnp.int32)
            for j in range(8):
                r = k * 8 + j
                g, w, s = lax.div(r, n_wave * PAIR), lax.rem(lax.div(r, PAIR), n_wave), lax.rem(r, PAIR)
                values = jnp.where(row == j, waves_ref[w * slots + g * PAIR + s], values)
            order[pl.ds(pl.multiple_of(k * 8, 8), 8), :] = values.astype(f32)

        loop(0, waves // 8, some)

    def build(t):
        points = points_ref[t]
        n = points.astype(f32)
        piece = 32
        inverse = 1.0 / jnp.full((1, longs), n, f32)
        lane = lax.broadcasted_iota(jnp.int32, (1, longs), 1)
        inside = jnp.where(lane < points, 1.0, 0.0) / math.sqrt(4.0 * waves)

        def some(k):
            base = pl.multiple_of(k * piece, piece)
            wave = order[pl.ds(base, piece), 0:1]
            product = wave * lane.astype(f32)
            turns = jnp.floor(product * inverse + 0.5)
            x = (product - turns * n) * inverse
            square = x * x
            gain = jnp.where(wave == 0.0, 1.0, 2.0) * inside
            table[t, pl.ds(base, piece), :] = (gain * horner(COS_TERMS, square)).astype(bf16)
            sine = (-gain) * (x * horner(SIN_TERMS, square))
            table[t, pl.ds(pl.multiple_of(waves + base, piece), piece), :] = sine.astype(bf16)

        loop(0, waves // piece, some)

    def scale_column(t, i):
        block = grid_scale_ref[:, pl.ds(pl.multiple_of(i * LEVELS, LEVELS), LEVELS)]
        band = lax.broadcasted_iota(jnp.int32, block.shape, 0)
        line = jnp.sum(jnp.where(band == band_ref[t], block, 0.0), axis=0, keepdims=True)
        square = (LEVELS, LEVELS)
        diagonal = lax.broadcasted_iota(jnp.int32, square, 0) == lax.broadcasted_iota(jnp.int32, square, 1)
        return jnp.sum(jnp.where(diagonal, line, 0.0), axis=1, keepdims=True)

    def grid(q):
        i = lax.rem(q, per)
        weight_copy(q).wait()

        @pl.when(q > 0)
        def _():
            inc_copy(q - 1).wait()

        loop(0, subs, lambda g: land_all(q * subs + g).wait())

        def one(t):
            scale = scale_column(t, i)
            parts = [land.at[q, p, t].reshape(waves, LEVELS)[...] for p in range(2)]
            synthesis = lax.dot_general(jnp.concatenate(parts, axis=0), table[t], (((0,), (0,)), ((), ())),
                                        preferred_element_type=f32)
            increment = (synthesis * scale).astype(bf16)
            ibuf[t] = increment
            weighted = increment.astype(f32) * wbuf[t].astype(f32) * scale
            adjoint = lax.dot_general(table[t], weighted.astype(bf16), (((1,), (1,)), ((), ())),
                                      preferred_element_type=f32).astype(bf16)
            for p in range(2):
                asend.at[q, p, t].reshape(waves, LEVELS)[...] = adjoint[p * waves:(p + 1) * waves]

        loop(0, lats, one)

        def send(g):
            u = q * subs + g

            @pl.when(u < units - 1)
            def _():
                loop(1, n_wave, lambda d: aland_copy(u, d).start())

            @pl.when(u == units - 1)
            def _():
                for p in range(2):
                    loop(1, n_wave, lambda d: aland_half(p, d).start())

            aland[u, :, me_w] = asend[q, :, :, g, me_w]

        loop(0, subs, send)
        inc_copy(q).start()

        @pl.when(q + 1 < chunks)
        def _():
            weight_copy(q + 1).start()

    def project(d, g, s, field):
        table_part = full[lax.rem(me_l + d, n_lev), g * PAIR + s]
        return jnp.dot(table_part, field, preferred_element_type=f32).astype(bf16)

    def adjoint_legendre(u):
        _, g, e, i = where_is(u)
        keep = lax.rem(u, RING)

        @pl.when(u < units - 1)
        def _():
            aland_all(u).wait()

        @pl.when(u < RING)
        def _():
            for d, p in lev_parts:
                out_copy(u + units - RING, d, p).wait_send()

        @pl.when(u >= RING)
        def _():
            for d, p in lev_parts:
                back_copy(u - RING, d, p).wait_send()

        for p in range(2):
            at = slice(p * LEVELS, (p + 1) * LEVELS)

            @pl.when(u == units - 1)
            def _():
                aland_half_all(p).wait()

            coef[p] = aland.at[u, p].reshape(lat_all * PAIR, LEVELS)[...].astype(f32)
            fields = [coef[p, pl.ds(s, lat_all, stride=PAIR), :].astype(bf16) for s in range(PAIR)]
            for d in lev_others:
                for s in range(PAIR):
                    away[keep, d - 1, s, :, at] = project(d, g, s, fields[s])
                back_copy(u, d, p).start()
            for s in range(PAIR):
                own[keep, s, :, at] = project(0, g, s, fields[s])

    def adjoint_vertical(u):
        _, g, e, i = where_is(u)
        slot, keep = lax.rem(u, PIECES), lax.rem(u, RING)
        @pl.when(u >= PIECES)
        def _():
            for d in range(n_lev):
                grad_copy(u - PIECES, d).wait()

        masks = [
            band_masks(own_wave(g, s) + row0 + lax.broadcasted_iota(jnp.int32, (rows, LEVELS), 0), waves)
            for s in range(PAIR)
        ]
        for d in range(n_lev):
            a, _ = level_block(d, i)
            matrix = mats[:, a].reshape(COV_BANDS * LEVELS, LEVELS)
            for p in range(2):
                if d > 0:
                    back_copy(u, d, p).wait_recv()
                for s in range(PAIR):
                    at = slice(p * LEVELS, (p + 1) * LEVELS)
                    x = own[keep, s, :, at] if d == 0 else back[u, d - 1, s, :, at]
                    stage[s, d, pl.ds(p, rows, stride=2), :] = banded_dot(x, masks[s], matrix)
            for s in range(PAIR):
                pieces.at[slot, d].reshape(PAIR, 2 * rows, LEVELS)[s] = stage[s, d].astype(bf16)
            grad_copy(u, d).start()

    for copy in small_copies():
        copy.start()
    mats_copy().start()
    for u in range(PIECES):
        for d in range(n_lev):
            x_copy(u, d).start()
    full_copy().start()
    weight_copy(0).start()
    barrier = greet(n_wave, n_lev)
    mats_copy().wait()
    for b in range(COV_BANDS):
        for a in range(variables):
            mats_t[a, b * LEVELS:(b + 1) * LEVELS, :] = mats[b, a].T
    for copy in small_copies():
        copy.wait()
    pl.semaphore_wait(barrier, n_wave + n_lev - 2)
    for d in lev_others:
        table_copy(0, d).start()

    def first(u):
        vertical(u)
        send_levels(u)

    loop(0, AHEAD, first)

    def front(u):
        legendre(u)

        @pl.when(u + AHEAD < units)
        def _():
            vertical(u + AHEAD)
            send_levels(u + AHEAD)

        @pl.when(u == subs - 1)
        def _():
            make_order()

        @pl.when((u >= subs) & (u - subs < lats))
        def _():
            build(u - subs)

    loop(0, units, front)
    loop(0, chunks, grid)

    def last(u):
        @pl.when(u < units)
        def _():
            adjoint_legendre(u)

        @pl.when(u > 0)
        def _():
            adjoint_vertical(u - 1)

    loop(0, units + 1, last)
    inc_copy(chunks - 1).wait()
    for u in range(units - PIECES, units):
        for d in range(n_lev):
            grad_copy(u, d).wait()

    def drain(u):
        for d, p in lev_parts:
            back_copy(units - RING + u, d, p).wait_send()

    loop(0, RING, drain)


def settle_kernel(inc_ref, grad_ref, inc_out, grad_out, a, b, a_in, a_out, b_in, b_out):
    def moves(i):
        return [
            (pltpu.make_async_copy(inc_ref.at[:, i], a.at[i], a_in.at[i]),
             pltpu.make_async_copy(a.at[i], inc_out.at[:, i], a_out.at[i])),
            (pltpu.make_async_copy(grad_ref.at[:, i], b.at[i], b_in.at[i]),
             pltpu.make_async_copy(b.at[i], grad_out.at[:, i], b_out.at[i])),
        ]

    steps = a.shape[0]
    stages = [moves(i) for i in range(steps)]
    for pairs in stages:
        for first, _ in pairs:
            first.start()
    for pairs in stages:
        for first, then in pairs:
            first.wait()
            then.start()
    for pairs in stages:
        for _, then in pairs:
            then.wait()


def settle(increment, gradient):
    hbm = pl.BlockSpec(memory_space=pl.ANY)
    dma = pltpu.SemaphoreType.DMA
    shapes = [increment.shape, gradient.shape]
    steps = increment.shape[1]
    kept = [pltpu.VMEM((steps, s[0], *s[2:]), jnp.bfloat16) for s in shapes]
    return pl.pallas_call(
        settle_kernel,
        out_shape=[jax.ShapeDtypeStruct(s, jnp.bfloat16) for s in shapes],
        in_specs=[hbm, hbm],
        out_specs=[hbm, hbm],
        scratch_shapes=[*kept, *[dma((steps,))] * 4],
        compiler_params=pltpu.CompilerParams(vmem_limit_bytes=VMEM_BYTES),
        name="settle",
    )(increment, gradient)


def shards_kernel(n_wave, n_lev, control, wave_of_slot, legendre, vertical, points, lat_band, grid_scale, obs_weight):
    members, slots, rows = control.shape[:3]
    waves = wave_of_slot.shape[0]
    variables = vertical.shape[1]
    columns = control.shape[4]
    cols = columns // n_lev
    lats, _, longs = obs_weight.shape
    chunks = members * variables // n_lev
    subs = slots // PAIR
    units = chunks * subs
    width = 2 * LEVELS
    bf16, f32 = jnp.bfloat16, jnp.float32
    hbm = pl.BlockSpec(memory_space=pl.ANY)
    dma = pltpu.SemaphoreType.DMA
    others = n_lev - 1
    half = (PAIR, rows, width)
    results = pl.pallas_call(
        functools.partial(transform_kernel, n_wave, n_lev),
        out_shape=[
            jax.ShapeDtypeStruct((members, lats, cols, longs), bf16),
            jax.ShapeDtypeStruct(control.shape, bf16),
        ],
        in_specs=[hbm] * 8,
        out_specs=[hbm, hbm],
        scratch_shapes=[
            pltpu.SMEM(wave_of_slot.shape, jnp.int32),
            pltpu.SMEM(points.shape, jnp.int32),
            pltpu.SMEM(lat_band.shape, jnp.int32),
            pltpu.VMEM(grid_scale.shape, f32),
            pltpu.VMEM((n_lev, *legendre.shape), bf16),
            pltpu.VMEM(vertical.shape, bf16),
            pltpu.VMEM((variables, COV_BANDS * LEVELS, LEVELS), bf16),
            pltpu.VMEM((waves, LEVELS), f32),
            pltpu.VMEM((PIECES, n_lev, PAIR, rows, 2, LEVELS), bf16),
            pltpu.VMEM((RING, *half), bf16),
            pltpu.VMEM((RING, others, *half), bf16),
            pltpu.VMEM((units, others, *half), bf16),
            pltpu.VMEM((units, others, *half), bf16),
            pltpu.VMEM((2, n_wave * lats * PAIR, LEVELS), f32),
            pltpu.VMEM((chunks, subs, 2, n_wave, lats, PAIR, LEVELS), bf16),
            pltpu.VMEM((chunks, 2, lats, subs, n_wave, PAIR, LEVELS), bf16),
            pltpu.VMEM((chunks, 2, lats, subs, n_wave, PAIR, LEVELS), bf16),
            pltpu.VMEM((units, 2, n_wave, lats, PAIR, LEVELS), bf16),
            pltpu.VMEM((lats, 2 * waves, longs), bf16),
            pltpu.VMEM((lats, LEVELS, longs), bf16),
            pltpu.VMEM((lats, LEVELS, longs), bf16),
            pltpu.VMEM((PAIR, n_lev, 2 * rows, LEVELS), f32),
            dma((4,)), dma, dma, dma((PIECES, n_lev)), dma, dma, dma((PIECES, n_lev)),
            dma((subs, others)), dma((subs, others)),
            *[dma((units, others, 2))] * 4,
            dma((units,)), dma((units,)), dma((units + 1,)), dma((units + 1,)),
        ],
        compiler_params=pltpu.CompilerParams(collective_id=0, has_side_effects=True, vmem_limit_bytes=VMEM_BYTES),
        name="transform",
    )(wave_of_slot, points, lat_band, grid_scale, vertical, control, legendre, obs_weight)
    return tuple(settle(*results))


def shards(n_wave, n_lev, *arrays):
    slots, rows, columns = arrays[0].shape[1], arrays[0].shape[2], arrays[0].shape[4]
    whole_tiles = slots % 16 == 0 and rows % 128 == 0 and columns % (n_lev * LEVELS) == 0
    if whole_tiles and n_lev > 1:
        return shards_kernel(n_wave, n_lev, *arrays)
    return shards_plain(*arrays)


def solution(mesh):
    in_specs = (
        P(None, "wave", "lev", None, None),
        P(),
        P("wave", "lev", None),
        P(),
        P("wave"),
        P("wave"),
        P(None, "lev"),
        P("wave", "lev", None),
    )
    out_specs = (P(None, "wave", "lev", None), P(None, "wave", "lev", None, None))
    body = functools.partial(shards, mesh.shape["wave"], mesh.shape["lev"])
    return jax.shard_map(body, mesh=mesh, in_specs=in_specs, out_specs=out_specs, check_vma=False)
```
